128 devices in a mesh: row: 2 (over core), col: 64 (over z, y, x).
Axes of the slice: x: 4, y: 4, z: 4, core: 2. Of those that a mesh axis runs over, the one named last changes fastest.
Arguments:
- v_panels: float32 [6144, 6144], P('row', 'col')
- t_factors: float32 [192, 32, 32], P('col')
- z_vectors: float32 [6144, 4096], P(None, ('col', 'row'))
Outputs:
- output: float32 [6144, 4096], P('row', 'col')
All inputs are finite; a program needn't handle non-finite values.
Results may differ from the reference program's by a relative error of at most 0.001.
Values sent between devices are 32-bit elements.
A program may use at most 1 GiB of HBM per device.

```python
import jax
import jax.numpy as jnp
from jax import lax

MAT_ORDER = 6144
PANEL_WIDTH = 32
ROW_DEVS = 2
COL_DEVS = 64
COLS_DEV = 32
NUM_PANELS = MAT_ORDER // PANEL_WIDTH
NUM_COLS = COLS_DEV * ROW_DEVS * COL_DEVS
HIGHEST = lax.Precision.HIGHEST


def compact_factors(panels):
    gram_mat = jnp.einsum('nja,njc->jac', panels, panels, precision=HIGHEST)
    diag_half = 0.5 * gram_mat * jnp.eye(PANEL_WIDTH, dtype=jnp.float32)
    upper_mat = jnp.triu(gram_mat, 1) + diag_half
    return jnp.triu(jnp.linalg.inv(upper_mat))


def to_stored(v_log):
    rows_perm = v_log.reshape(NUM_PANELS // ROW_DEVS, ROW_DEVS, PANEL_WIDTH, MAT_ORDER)
    rows_perm = rows_perm.transpose(1, 0, 2, 3).reshape(MAT_ORDER, NUM_PANELS // COL_DEVS, COL_DEVS, PANEL_WIDTH)
    return rows_perm.transpose(0, 2, 1, 3).reshape(MAT_ORDER, MAT_ORDER)


def setup_inputs(seed: int = 0) -> dict:
    root_key = jax.random.key(seed)
    key_v, key_z = jax.random.split(root_key)
    below_diag = jax.random.normal(key_v, (MAT_ORDER, MAT_ORDER), jnp.float32)
    v_log = jnp.tril(below_diag, -1) + jnp.eye(MAT_ORDER, dtype=jnp.float32)
    t_log = compact_factors(v_log.reshape(MAT_ORDER, NUM_PANELS, PANEL_WIDTH))
    t_st = t_log.reshape(NUM_PANELS // COL_DEVS, COL_DEVS, PANEL_WIDTH, PANEL_WIDTH)
    t_st = t_st.transpose(1, 0, 2, 3).reshape(NUM_PANELS, PANEL_WIDTH, PANEL_WIDTH)
    z_draw = jax.random.normal(key_z, (MAT_ORDER, NUM_COLS), jnp.float32)
    return {'v_panels': to_stored(v_log), 't_factors': t_st, 'z_vectors': z_draw}


def reference(v_panels, t_factors, z_vectors):
    panels = v_panels.reshape(MAT_ORDER, COL_DEVS, NUM_PANELS // COL_DEVS, PANEL_WIDTH)
    panels = panels.transpose(2, 1, 0, 3).reshape(NUM_PANELS, MAT_ORDER, PANEL_WIDTH)
    factors = t_factors.reshape(COL_DEVS, NUM_PANELS // COL_DEVS, PANEL_WIDTH, PANEL_WIDTH)
    factors = factors.transpose(1, 0, 2, 3).reshape(NUM_PANELS, PANEL_WIDTH, PANEL_WIDTH)

    def apply_panel(x_cur, panel_item):
        v_j, t_j = panel_item
        w_mat = jnp.dot(v_j.T, x_cur, precision=HIGHEST, preferred_element_type=jnp.float32)
        y_mat = jnp.dot(t_j, w_mat, precision=HIGHEST, preferred_element_type=jnp.float32)
        x_new = x_cur - jnp.dot(v_j, y_mat, precision=HIGHEST, preferred_element_type=jnp.float32)
        return x_new, None

    return lax.scan(apply_panel, z_vectors, (panels, factors), reverse=True)[0]
```

```python
import functools

import jax
import jax.numpy as jnp
from jax import lax
from jax.experimental import pallas as pl
from jax.experimental.pallas import tpu as pltpu
from jax.sharding import PartitionSpec as P

HIGHEST = lax.Precision.HIGHEST
BLOCK = 256
CHUNK = 512


def dot_nn(a, b):
    return lax.dot_general(a, b, (((1,), (0,)), ((), ())), precision=HIGHEST, preferred_element_type=jnp.float32)


def dot_nt(a, b):
    return lax.dot_general(a, b, (((1,), (1,)), ((), ())), precision=HIGHEST, preferred_element_type=jnp.float32)


def group_kernel(dims, vt_hbm, xin_ref, out_ref, vbuf, part, other, v_sem, send_sem, recv_sem):
    blocks, rows, first_row, step_rows, width, chunk = dims
    cols = xin_ref.shape[0]
    mate = 1 - lax.axis_index('row')

    barrier = pltpu.get_barrier_semaphore()
    pl.semaphore_signal(barrier, inc=1, device_id={'row': mate}, device_id_type=pl.DeviceIdType.MESH)
    pl.semaphore_wait(barrier, 1)

    def fetch(blk, slot):
        src = vt_hbm.at[pl.ds(pl.multiple_of(blk * BLOCK, BLOCK), BLOCK), :]
        return pltpu.make_async_copy(src, vbuf.at[slot], v_sem.at[slot])

    fetch(blocks - 1, 0).start()
    out_ref[...] = xin_ref[...]

    row_id = lax.broadcasted_iota(jnp.int32, (BLOCK, BLOCK), 0)
    col_id = lax.broadcasted_iota(jnp.int32, (BLOCK, BLOCK), 1)

    def block_step(step, carry):
        blk = blocks - 1 - step
        slot = lax.rem(step, 2)
        fetch(blk, slot).wait()

        @pl.when(step + 1 < blocks)
        def _():
            fetch(blk - 1, 1 - slot).start()

        start = (blk * step_rows) // chunk
        part[slot] = jnp.zeros(part.shape[1:], jnp.float32)

        def gather_products(c, carry):
            at = pl.multiple_of(c * chunk, chunk)
            v_c = vbuf[slot, :, pl.ds(at, chunk)]
            x_c = out_ref[:, pl.ds(first_row + at, chunk)]
            part[slot] += dot_nt(jnp.concatenate([x_c, v_c], axis=0), v_c)
            return carry

        lax.fori_loop(start, rows // chunk, gather_products, 0)

        swap = pltpu.make_async_remote_copy(
            src_ref=part.at[slot], dst_ref=other.at[slot], send_sem=send_sem.at[slot], recv_sem=recv_sem.at[slot],
            device_id={'row': mate}, device_id_type=pl.DeviceIdType.MESH)
        swap.start()
        swap.wait()

        w_t = part[slot, :cols] + other[slot, :cols]
        gram = part[slot, cols:] + other[slot, cols:]
        t_rows = vbuf[slot, :, rows:rows + 128]
        t_mat = jnp.concatenate([t_rows, t_rows], axis=1)
        t_mat = jnp.where(row_id // width == col_id // width, t_mat, 0.0)
        size = width
        while size < BLOCK:
            pick = (row_id // size + 1 == col_id // size) & (row_id // (2 * size) == col_id // (2 * size))
            t_mat = t_mat - dot_nn(dot_nn(t_mat, jnp.where(pick, gram, 0.0)), t_mat)
            size *= 2
        y_t = dot_nt(w_t, t_mat)

        def update(c, carry):
            at = pl.multiple_of(c * chunk, chunk)
            out_ref[:, pl.ds(first_row + at, chunk)] -= dot_nn(y_t, vbuf[slot, :, pl.ds(at, chunk)])
            return carry

        lax.fori_loop(start, rows // chunk, update, 0)
        return carry

    lax.fori_loop(0, blocks, block_step, 0)


def apply_group(x_t, vt, group, width, row_devs):
    cols, local_rows = x_t.shape
    group_cols, padded = vt.shape
    rows = padded - 128
    chunk = next(size for size in (CHUNK, 256, 128) if rows % size == 0)
    blocks = group_cols // BLOCK
    dims = (blocks, rows, local_rows - rows, BLOCK // row_devs, width, chunk)
    flops = 12 * blocks * rows * BLOCK * (BLOCK + 2 * cols)
    return pl.pallas_call(
        functools.partial(group_kernel, dims),
        out_shape=jax.ShapeDtypeStruct(x_t.shape, jnp.float32),
        in_specs=[pl.BlockSpec(memory_space=pl.ANY), pl.BlockSpec(memory_space=pltpu.VMEM)],
        out_specs=pl.BlockSpec(memory_space=pltpu.VMEM),
        scratch_shapes=[
            pltpu.VMEM((2, BLOCK, padded), jnp.float32),
            pltpu.VMEM((2, cols + BLOCK, BLOCK), jnp.float32),
            pltpu.VMEM((2, cols + BLOCK, BLOCK), jnp.float32),
            pltpu.SemaphoreType.DMA((2,)),
            pltpu.SemaphoreType.DMA((2,)),
            pltpu.SemaphoreType.DMA((2,)),
        ],
        cost_estimate=pl.CostEstimate(flops=flops, bytes_accessed=4 * group_cols * padded, transcendentals=0),
        compiler_params=pltpu.CompilerParams(collective_id=group, has_side_effects=True,
                                             vmem_limit_bytes=40 * 1024 * 1024),
    )(vt, x_t)


def solution(mesh):
    row_devs = mesh.shape['row']
    col_devs = mesh.shape['col']

    def local_apply(v_loc, t_loc, z_loc):
        groups, width = t_loc.shape[0], t_loc.shape[1]
        local_rows = v_loc.shape[0]
        gathered = {}
        for group in reversed(range(groups)):
            first_row = group * col_devs * width // row_devs
            v_t = v_loc[first_row:, group * width:(group + 1) * width].T
            op = jnp.concatenate([v_t, jnp.tile(t_loc[group], (1, 128 // width))], axis=1)
            gathered[group] = lax.all_gather(op, 'col', axis=0, tiled=True)
        x_t = lax.all_to_all(z_loc.T, 'row', 1, 0, tiled=True)
        for group in reversed(range(groups)):
            x_t = apply_group(x_t, gathered[group], group, width, row_devs)
        return x_t.T

    return jax.shard_map(local_apply, mesh=mesh,
                         in_specs=(P('row', 'col'), P('col', None, None), P(None, ('col', 'row'))),
                         out_specs=P('row', 'col'), check_vma=False)
```

```python
import functools

import jax
import jax.numpy as jnp
from jax import lax
from jax.experimental import pallas as pl
from jax.experimental.pallas import tpu as pltpu
from jax.sharding import PartitionSpec as P

HIGHEST = lax.Precision.HIGHEST
MESH = pl.DeviceIdType.MESH
BLOCK = 256
TILE = 128
CHUNK = 4
SIDE = 4
WIDTH = 32
TILES = {2: 8, 1: 16, 0: 24}
ORDERS = ((2, 1, 0), (1, 0, 2), (0, 2, 1))
RANGES = {
    2: ((7, 9), (0, 6), (6, 7)),
    1: ((13, 16), (0, 8), (8, 13)),
    0: ((17, 24), (0, 9), (9, 17)),
}


def dot_nn(a, b):
    return lax.dot_general(a, b, (((1,), (0,)), ((), ())), precision=HIGHEST, preferred_element_type=jnp.float32)


def dot_nt(a, b):
    return lax.dot_general(a, b, (((1,), (1,)), ((), ())), precision=HIGHEST, preferred_element_type=jnp.float32)


def regions(group, part, phase, coords, pos, half):
    order = ORDERS[part]
    low, high = RANGES[group][part]
    index = list(coords)
    index[order[phase]] = pos
    for axis in order[:phase]:
        index[axis] = pl.ds(0, SIDE)
    if half is not None:
        if phase == 0:
            middle = (low + high + 1) // 2
            low, high = ((low, middle), (middle, high))[half]
        else:
            index[order[0]] = pl.ds(2 * half, 2)
    if phase == 2 and part == 1:
        spans = [(z, max(low, 2 * z)) for z in range(SIDE)]
        return [(z, index[1], index[2], pl.ds(first, high - first)) for z, first in spans if first < high]
    if low == high:
        return []
    return [(*index, pl.ds(low, high - low))]


def semaphore_table():
    table = {}
    for group in TILES:
        for part in range(3):
            for phase in range(3):
                for stage in range(2):
                    for way in range(2):
                        half = way if stage else None
                        for i in range(len(regions(group, part, phase, (0, 0, 0), 0, half))):
                            table[group, part, phase, stage, way, i] = len(table)
    return table


TABLE = semaphore_table()


def kernel(v_hbm, t_tile, z_hbm, out_ref, buf2, buf1, buf0, x_buf, part_buf, other, load_sem, x_sem, send_sem, recv_sem,
           swap_send, swap_recv):
    bufs = {2: buf2, 1: buf1, 0: buf0}
    cols, local_rows = x_buf.shape
    share = cols // 2
    me = lax.axis_index('row')
    mate = 1 - me
    chip = lax.axis_index('col')
    coords = (chip // (SIDE * SIDE), lax.rem(chip // SIDE, SIDE), lax.rem(chip, SIDE))
    strides = (SIDE * SIDE, SIDE, 1)

    def shifted(axis, by):
        return lax.rem(coords[axis] + by + SIDE, SIDE)

    def neighbour(axis, by):
        return {'col': chip + (shifted(axis, by) - coords[axis]) * strides[axis]}

    for group in TILES:
        for z in range(1, SIDE):
            count = 2 * z
            shape = (SIDE, SIDE, count, WIDTH, TILE)
            bufs[group][z, :, :, 0:count, :, :] = jnp.zeros(shape, jnp.float32)

    barrier = pltpu.get_barrier_semaphore()
    pl.semaphore_signal(barrier, inc=1, device_id={'row': mate}, device_id_type=MESH)
    for axis in range(3):
        for by in (1, -1):
            pl.semaphore_signal(barrier, inc=1, device_id=neighbour(axis, by), device_id_type=MESH)
    pl.semaphore_wait(barrier, 7)

    own = {group: bufs[group].at[coords[0], coords[1], coords[2]] for group in TILES}
    for group, tiles in TILES.items():
        first = local_rows - tiles * TILE
        for tile in range(tiles):
            src = v_hbm.at[pl.ds(group * WIDTH, WIDTH), pl.ds(first + tile * TILE, TILE)]
            pltpu.make_async_copy(src, own[group].at[tile], load_sem.at[group]).start()
    pltpu.make_async_copy(t_tile, own[2].at[TILES[2]], load_sem.at[2]).start()

    keep = pltpu.make_async_copy(z_hbm.at[:, pl.ds(pl.multiple_of(me * local_rows, TILE), local_rows)],
                                 x_buf.at[pl.ds(pl.multiple_of(me * share, 8), share), :], x_sem.at[0])
    give = pltpu.make_async_remote_copy(
        src_ref=z_hbm.at[:, pl.ds(pl.multiple_of(mate * local_rows, TILE), local_rows)],
        dst_ref=x_buf.at[pl.ds(pl.multiple_of(me * share, 8), share), :],
        send_sem=x_sem.at[1], recv_sem=x_sem.at[2], device_id={'row': mate}, device_id_type=MESH)
    take = pltpu.make_async_remote_copy(
        src_ref=z_hbm.at[:, pl.ds(pl.multiple_of(mate * local_rows, TILE), local_rows)],
        dst_ref=x_buf.at[pl.ds(pl.multiple_of(mate * share, 8), share), :],
        send_sem=x_sem.at[1], recv_sem=x_sem.at[2], device_id={'row': mate}, device_id_type=MESH)

    def messages(group, phase, stage, incoming):
        copies = []
        for part in range(3):
            axis = ORDERS[part][phase]
            for way in range(2):
                sign = 1 - 2 * way
                behind = (-sign if stage else 0) + (-sign if incoming else 0)
                pos = shifted(axis, behind)
                half = way if stage else None
                for i, index in enumerate(regions(group, part, phase, coords, pos, half)):
                    number = TABLE[group, part, phase, stage, way, i]
                    ref = bufs[group].at[index]
                    copies.append(pltpu.make_async_remote_copy(
                        src_ref=ref, dst_ref=ref, send_sem=send_sem.at[number], recv_sem=recv_sem.at[number],
                        device_id=neighbour(axis, sign), device_id_type=MESH))
        return copies

    def send(group, phase, stage):
        for copy in messages(group, phase, stage, False):
            copy.start()

    def receive(group, phase, stage):
        for copy in messages(group, phase, stage, True):
            copy.wait_recv()

    def relay(group, phase, stage):
        receive(group, phase, stage)
        if stage == 0:
            send(group, phase, 1)
        elif phase < 2:
            send(group, phase + 1, 0)

    def loaded(group):
        pltpu.make_async_copy(own[group], own[group], load_sem.at[group]).wait()

    loaded(2)
    send(2, 0, 0)
    keep.start()
    give.start()
    loaded(1)
    loaded(0)
    relay(2, 0, 0)
    send(1, 0, 0)
    relay(2, 0, 1)
    relay(1, 0, 0)
    relay(2, 1, 0)
    send(0, 0, 0)
    relay(2, 1, 1)
    relay(1, 0, 1)
    relay(0, 0, 0)
    relay(2, 2, 0)
    relay(1, 1, 0)
    relay(1, 1, 1)
    relay(0, 0, 1)
    receive(2, 2, 1)
    keep.wait()
    take.wait_recv()

    row_id = lax.broadcasted_iota(jnp.int32, (BLOCK, BLOCK), 0)
    col_id = lax.broadcasted_iota(jnp.int32, (BLOCK, BLOCK), 1)

    def apply_group(group, events):
        buf = bufs[group]
        tiles = TILES[group]
        first_row = local_rows - tiles * TILE

        def block_step(step, carry):
            blk = 7 - step
            z, y = blk // 2, 2 * lax.rem(blk, 2)
            slot = lax.rem(step, 2)

            def tile_of(ref, tile):
                return ref[z, pl.ds(y, 2), :, tile].reshape(BLOCK, TILE)

            def chunk_of(c):
                return jnp.concatenate([tile_of(buf, c * CHUNK + i) for i in range(CHUNK)], axis=1)

            def rows_of(c):
                return pl.ds(pl.multiple_of(first_row + c * (CHUNK * TILE), TILE), CHUNK * TILE)

            start = blk // CHUNK
            part_buf[slot] = jnp.zeros(part_buf.shape[1:], jnp.float32)

            def products(c, carry):
                v_c = chunk_of(c)
                part_buf[slot] += dot_nt(jnp.concatenate([x_buf[:, rows_of(c)], v_c], axis=0), v_c)
                return carry

            lax.fori_loop(start, tiles // CHUNK, products, 0)

            swap = pltpu.make_async_remote_copy(
                src_ref=part_buf.at[slot], dst_ref=other.at[slot], send_sem=swap_send.at[slot],
                recv_sem=swap_recv.at[slot], device_id={'row': mate}, device_id_type=MESH)
            swap.start()
            swap.wait()

            w_t = part_buf[slot, :cols] + other[slot, :cols]
            gram = part_buf[slot, cols:] + other[slot, cols:]
            t_rows = tile_of(buf2, TILES[2])[:, group * WIDTH:(group + 1) * WIDTH]
            t_mat = jnp.concatenate([t_rows] * (BLOCK // WIDTH), axis=1)
            t_mat = jnp.where(row_id // WIDTH == col_id // WIDTH, t_mat, 0.0)
            size = WIDTH
            while size < BLOCK:
                pick = (row_id // size + 1 == col_id // size) & (row_id // (2 * size) == col_id // (2 * size))
                t_mat = t_mat - dot_nn(dot_nn(t_mat, jnp.where(pick, gram, 0.0)), t_mat)
                size *= 2
            y_t = dot_nt(w_t, t_mat)

            def update(c, carry):
                x_buf[:, rows_of(c)] -= dot_nn(y_t, chunk_of(c))
                return carry

            lax.fori_loop(start, tiles // CHUNK, update, 0)

            for when, event in events.items():
                @pl.when(step == when)
                def _():
                    relay(*event)

            return carry

        lax.fori_loop(0, 8, block_step, 0)

    apply_group(2, {1: (0, 1, 0), 3: (1, 2, 0), 5: (0, 1, 1)})
    receive(1, 2, 1)
    apply_group(1, {4: (0, 2, 0)})
    receive(0, 2, 1)
    apply_group(0, {})
    out_ref[...] = x_buf[...]

    give.wait_send()
    for group in TILES:
        for phase in range(3):
            for stage in range(2):
                for copy in messages(group, phase, stage, False):
                    copy.wait_send()


def solution(mesh):
    def local_apply(v_loc, t_loc, z_loc):
        groups, width = t_loc.shape[0], t_loc.shape[1]
        local_rows = v_loc.shape[0]
        share = z_loc.shape[1]
        t_tile = jnp.pad(t_loc.transpose(1, 0, 2).reshape(width, groups * width), ((0, 0), (0, TILE - groups * width)))
        cols = 2 * share
        any_spec = pl.BlockSpec(memory_space=pl.ANY)

        def buffer(tiles):
            return pltpu.VMEM((SIDE, SIDE, SIDE, tiles, WIDTH, TILE), jnp.float32)

        x_t = pl.pallas_call(
            kernel,
            out_shape=jax.ShapeDtypeStruct((cols, local_rows), jnp.float32),
            in_specs=[any_spec, any_spec, any_spec],
            out_specs=pl.BlockSpec(memory_space=pltpu.VMEM),
            scratch_shapes=[
                buffer(TILES[2] + 1),
                buffer(TILES[1]),
                buffer(TILES[0]),
                pltpu.VMEM((cols, local_rows), jnp.float32),
                pltpu.VMEM((2, cols + BLOCK, BLOCK), jnp.float32),
                pltpu.VMEM((2, cols + BLOCK, BLOCK), jnp.float32),
                pltpu.SemaphoreType.DMA((3,)),
                pltpu.SemaphoreType.DMA((3,)),
                pltpu.SemaphoreType.DMA((len(TABLE),)),
                pltpu.SemaphoreType.DMA((len(TABLE),)),
                pltpu.SemaphoreType.DMA((2,)),
                pltpu.SemaphoreType.DMA((2,)),
            ],
            compiler_params=pltpu.CompilerParams(collective_id=0, has_side_effects=True, vmem_limit_bytes=67043328),
        )(v_loc.T, t_tile, z_loc.T)
        return x_t.T

    return jax.shard_map(local_apply, mesh=mesh,
                         in_specs=(P('row', 'col'), P('col', None, None), P(None, ('col', 'row'))),
                         out_specs=P('row', 'col'), check_vma=False)
```

```python
import functools

import jax
import jax.numpy as jnp
from jax import lax
from jax.experimental import pallas as pl
from jax.experimental.pallas import tpu as pltpu
from jax.sharding import PartitionSpec as P

HIGHEST = lax.Precision.HIGHEST
MESH = pl.DeviceIdType.MESH
BLOCK = 256
HALF = BLOCK // 2
TILE = 128
CHUNK = 4
SIDE = 4
WIDTH = 32
TILES = {2: 8, 1: 16, 0: 24}
EXTRA = {2: 1, 1: 0, 0: 1}
OWNER = 0
QUARTER = TILES[OWNER] // SIDE * TILE
ORDERS = ((2, 1, 0), (1, 0, 2), (0, 2, 1))
RANGES = {
    2: ((7, 9), (0, 6), (6, 7)),
    1: ((12, 16), (0, 8), (8, 12)),
    0: ((20, 25), (0, 11), (11, 20)),
}
STREAMED = 0


def dot_nn(a, b):
    return lax.dot_general(a, b, (((1,), (0,)), ((), ())), precision=HIGHEST, preferred_element_type=jnp.float32)


def dot_nt(a, b):
    return lax.dot_general(a, b, (((1,), (1,)), ((), ())), precision=HIGHEST, preferred_element_type=jnp.float32)


def regions(group, part, phase, plane, coords, pos, half):
    order = ORDERS[part]
    low, high = RANGES[group][part]
    index = list(coords)
    index[order[phase]] = pos
    for axis in order[:phase]:
        index[axis] = pl.ds(0, SIDE)
    if phase == 0:
        middle = (low + high + 1) // 2
        low, high = ((low, middle), (middle, high))[half]
    else:
        index[order[1 if plane is not None and order[0] == 0 else 0]] = pl.ds(2 * half, 2)
    if phase == 2 and part > 0 and (part == 1 or plane is not None):
        planes = range(SIDE) if plane is None else (plane,)
        spans = [(z, max(low, 2 * z) if part == 1 else low) for z in planes]
        return [(z, index[1], index[2], pl.ds(first, high - first)) for z, first in spans if first < high]
    if low == high:
        return []
    return [(*index, pl.ds(low, high - low))]


def parts_of(group, phase, plane):
    if group != STREAMED or phase < 2:
        return (0, 1, 2)
    return (0,) if plane is None else (1, 2)


def planes_of(group, phase):
    return (None, 3, 2, 1, 0) if group == STREAMED and phase == 2 else (None,)


def message_keys():
    for group in TILES:
        for phase in range(3):
            for plane in planes_of(group, phase):
                for piece in range(3):
                    yield group, phase, plane, piece


def half_of(piece, way):
    return 1 - way if piece == 1 else way


def semaphore_table():
    table = {}
    for group, phase, plane, piece in message_keys():
        for part in parts_of(group, phase, plane):
            for way in range(2):
                for i in range(len(regions(group, part, phase, plane, (0, 0, 0), 0, half_of(piece, way)))):
                    table[group, phase, plane, piece, part, way, i] = len(table)
    return table


TABLE = semaphore_table()


def kernel(v_hbm, t_hbm, z_hbm, out_ref, buf2, buf1, buf0, x_buf, w_part, w_other, g_part, g_other, quarters, t_line,
           line_part, line_other, line_half, line_gram, line_t,
           load_sem, x_sem, send_sem, recv_sem, swap_send, swap_recv, line_send, line_recv, line_load):
    bufs = {2: buf2, 1: buf1, 0: buf0}
    cols, local_rows = x_buf.shape
    share = cols // 2
    me = lax.axis_index('row')
    mate = 1 - me
    chip = lax.axis_index('col')
    coords = (chip // (SIDE * SIDE), lax.rem(chip // SIDE, SIDE), lax.rem(chip, SIDE))
    strides = (SIDE * SIDE, SIDE, 1)
    my_x = coords[2]

    def shifted(axis, by):
        return lax.rem(coords[axis] + by + SIDE, SIDE)

    def neighbour(axis, by):
        return {'col': chip + (shifted(axis, by) - coords[axis]) * strides[axis]}

    def to_mate(src, dst, send, recv):
        return pltpu.make_async_remote_copy(src_ref=src, dst_ref=dst, send_sem=send, recv_sem=recv,
                                            device_id={'row': mate}, device_id_type=MESH)

    for group in TILES:
        for z in range(1, SIDE):
            shape = (SIDE, SIDE, 2 * z, WIDTH, TILE)
            bufs[group][z, :, :, 0:2 * z, :, :] = jnp.zeros(shape, jnp.float32)

    barrier = pltpu.get_barrier_semaphore()
    pl.semaphore_signal(barrier, inc=1, device_id={'row': mate}, device_id_type=MESH)
    for axis, by in ((0, 1), (0, -1), (1, 1), (1, -1), (2, 1), (2, 2), (2, 3)):
        pl.semaphore_signal(barrier, inc=1, device_id=neighbour(axis, by), device_id_type=MESH)
    pl.semaphore_wait(barrier, 8)

    own = {group: bufs[group].at[coords[0], coords[1], coords[2]] for group in TILES}

    def load(group):
        first = local_rows - TILES[group] * TILE
        for tile in range(TILES[group]):
            src = v_hbm.at[pl.ds(group * WIDTH, WIDTH), pl.ds(first + tile * TILE, TILE)]
            pltpu.make_async_copy(src, own[group].at[tile], load_sem.at[group]).start()
        if group == 2:
            pltpu.make_async_copy(t_hbm, own[2].at[TILES[2]], load_sem.at[2]).start()

    def loaded(group):
        tiles = pl.ds(0, TILES[group] + (1 if group == 2 else 0))
        pltpu.make_async_copy(own[group].at[tiles], own[group].at[tiles], load_sem.at[group]).wait()

    mine = pl.ds(pl.multiple_of(me * local_rows, TILE), local_rows)
    theirs = pl.ds(pl.multiple_of(mate * local_rows, TILE), local_rows)
    my_cols = x_buf.at[pl.ds(pl.multiple_of(me * share, 8), share), :]
    their_cols = x_buf.at[pl.ds(pl.multiple_of(mate * share, 8), share), :]
    keep = pltpu.make_async_copy(z_hbm.at[:, mine], my_cols, x_sem.at[0])
    give = to_mate(z_hbm.at[:, theirs], my_cols, x_sem.at[1], x_sem.at[2])
    take = to_mate(z_hbm.at[:, theirs], their_cols, x_sem.at[1], x_sem.at[2])

    def messages(group, phase, plane, piece, incoming):
        copies = []
        for part in parts_of(group, phase, plane):
            axis = ORDERS[part][phase]
            for way in range(2):
                sign = 1 - 2 * way
                pos = shifted(axis, (-sign if piece == 2 else 0) + (-sign if incoming else 0))
                for i, index in enumerate(regions(group, part, phase, plane, coords, pos, half_of(piece, way))):
                    number = TABLE[group, phase, plane, piece, part, way, i]
                    ref = bufs[group].at[index]
                    copies.append(pltpu.make_async_remote_copy(
                        src_ref=ref, dst_ref=ref, send_sem=send_sem.at[number], recv_sem=recv_sem.at[number],
                        device_id=neighbour(axis, sign), device_id_type=MESH))
        return copies

    def begin(group, phase, plane=None):
        for piece in range(2):
            for copy in messages(group, phase, plane, piece, False):
                copy.start()

    def forward(group, phase, plane=None):
        for copy in messages(group, phase, plane, 0, True):
            copy.wait_recv()
        for copy in messages(group, phase, plane, 2, False):
            copy.start()

    def finish(group, phase, plane=None):
        for piece in range(1, 3):
            for copy in messages(group, phase, plane, piece, True):
                copy.wait_recv()

    def advance(group, phase):
        finish(group, phase)
        begin(group, phase + 1)
        if group == STREAMED and phase == 1:
            begin(group, 2, 3)
            begin(group, 2, 2)

    def quarter(x):
        return v_hbm.at[pl.ds(OWNER * WIDTH, WIDTH), pl.ds(pl.multiple_of(x * QUARTER, TILE), QUARTER)]

    def line_copies(kind, incoming):
        copies = []
        for by in range(1, SIDE):
            other = shifted(2, by)
            slot = shifted(2, -by) if incoming else my_x
            src, dst = {
                0: (quarter(other), quarters.at[slot]),
                1: (t_hbm, t_line.at[slot]),
                2: (line_half.at[my_x], line_half.at[slot]),
            }[kind]
            copies.append(pltpu.make_async_remote_copy(
                src_ref=src, dst_ref=dst, send_sem=line_send.at[kind, by - 1], recv_sem=line_recv.at[kind, by - 1],
                device_id=neighbour(2, by), device_id_type=MESH))
        return copies

    own_quarter = pltpu.make_async_copy(quarter(my_x), quarters.at[my_x], line_load.at[0])
    own_t = pltpu.make_async_copy(t_hbm, t_line.at[my_x], line_load.at[1])
    swap_line = to_mate(line_part, line_other, line_send.at[3, 0], line_recv.at[3, 0])
    my_half = pl.ds(pl.multiple_of(me * (HALF // 2), 8), HALF // 2)
    their_half = pl.ds(pl.multiple_of(mate * (HALF // 2), 8), HALF // 2)
    give_half = to_mate(line_gram.at[my_half, :], line_gram.at[my_half, :], line_send.at[3, 1], line_recv.at[3, 1])
    take_half = to_mate(line_gram.at[my_half, :], line_gram.at[their_half, :], line_send.at[3, 1], line_recv.at[3, 1])

    def block_diagonal(t_rows, group):
        size = t_rows.shape[0]
        column = t_rows[:, group * WIDTH:(group + 1) * WIDTH]
        wide = jnp.concatenate([column] * (size // WIDTH), axis=1)
        row_id = lax.broadcasted_iota(jnp.int32, (size, size), 0)
        col_id = lax.broadcasted_iota(jnp.int32, (size, size), 1)
        return jnp.where(row_id // WIDTH == col_id // WIDTH, wide, 0.0), row_id, col_id

    def merged(t_rows, group, gram):
        t_mat, row_id, col_id = block_diagonal(t_rows, group)
        size = WIDTH
        while size < gram.shape[0]:
            pick = (row_id // size + 1 == col_id // size) & (row_id // (2 * size) == col_id // (2 * size))
            t_mat = t_mat - dot_nn(dot_nn(t_mat, jnp.where(pick, gram, 0.0)), t_mat)
            size *= 2
        return t_mat

    def line_1():
        for kind in range(2):
            for copy in line_copies(kind, True):
                copy.wait_recv()
        own_quarter.wait()
        own_t.wait()
        q = quarters[...].reshape(HALF, QUARTER)
        line_part[...] = dot_nt(q, q)
        swap_line.start()

    def line_2():
        swap_line.wait_recv()
        line_half[my_x] = line_part[my_half, :] + line_other[my_half, :]
        for copy in line_copies(2, False):
            copy.start()

    def line_3():
        for copy in line_copies(2, True):
            copy.wait_recv()
        line_gram[my_half, :] = (line_half[0] + line_half[1]) + (line_half[2] + line_half[3])
        give_half.start()

    def line_4():
        take_half.wait_recv()
        line_t[...] = merged(t_line[...].reshape(HALF, TILE), OWNER, line_gram[...])
        bufs[OWNER][coords[0], coords[1], coords[2], TILES[OWNER]] = line_t[pl.ds(pl.multiple_of(my_x * WIDTH, 8), WIDTH), :]

    load(2)
    for kind in range(2):
        for copy in line_copies(kind, False):
            copy.start()
    own_quarter.start()
    own_t.start()
    load(1)
    loaded(2)
    begin(2, 0)
    load(0)
    keep.start()
    give.start()
    loaded(1)
    begin(1, 0)
    loaded(0)
    forward(2, 0)
    line_1()
    forward(1, 0)
    advance(2, 0)
    line_2()
    line_3()
    line_4()
    forward(2, 1)
    advance(2, 1)
    begin(0, 0)
    advance(1, 0)
    forward(2, 2)
    forward(0, 0)
    forward(1, 1)
    finish(2, 2)
    keep.wait()
    take.wait_recv()

    def apply_group(group, before, middle):
        buf = bufs[group]
        tiles = TILES[group]
        first_row = local_rows - tiles * TILE

        def block_step(step, carry):
            blk = 7 - step
            z, y = blk // 2, 2 * lax.rem(blk, 2)
            slot = lax.rem(step, 2)

            for when, events in before.items():
                @pl.when(step == when)
                def _():
                    for event in events:
                        event()

            def run_middle():
                for when, events in middle.items():
                    @pl.when(step == when)
                    def _():
                        for event in events:
                            event()

            def chunk_of(c):
                pieces = [buf[z, pl.ds(y, 2), :, c * CHUNK + i].reshape(BLOCK, TILE) for i in range(CHUNK)]
                return jnp.concatenate(pieces, axis=1)

            def rows_of(c):
                return pl.ds(pl.multiple_of(first_row + c * (CHUNK * TILE), TILE), CHUNK * TILE)

            def over_chunks(body):
                lax.fori_loop(blk // CHUNK, tiles // CHUNK, lambda c, carry: (body(c), carry)[1], 0)

            if group == OWNER:
                w_part[slot] = jnp.zeros(w_part.shape[1:], jnp.float32)

                def products(c):
                    v_c = chunk_of(c)
                    w_part[slot] += dot_nt(jnp.concatenate([x_buf[:, rows_of(c)], v_c[:HALF]], axis=0), v_c)

                over_chunks(products)
                swap = to_mate(w_part.at[slot], w_other.at[slot], swap_send.at[0, slot], swap_recv.at[0, slot])
                swap.start()
                run_middle()
                swap.wait()
                total = w_part[slot] + w_other[slot]
                w_1, w_2 = total[:cols, :HALF], total[:cols, HALF:]
                cross = total[cols:, HALF:]
                t_1 = buf[z, y, :, tiles].reshape(HALF, TILE)
                t_2 = buf[z, y + 1, :, tiles].reshape(HALF, TILE)
                y_2 = dot_nt(w_2, t_2)
                y_1 = dot_nt(w_1 - dot_nt(y_2, cross), t_1)
                y_t = jnp.concatenate([y_1, y_2], axis=1)
            else:
                g_part[slot] = jnp.zeros(g_part.shape[1:], jnp.float32)

                def gram_products(c):
                    v_c = chunk_of(c)
                    g_part[slot] += dot_nt(v_c, v_c)

                over_chunks(gram_products)
                g_swap = to_mate(g_part.at[slot], g_other.at[slot], swap_send.at[1, slot], swap_recv.at[1, slot])
                g_swap.start()
                w_rows = pl.ds(0, cols)
                w_part[slot, w_rows] = jnp.zeros((cols, BLOCK), jnp.float32)

                def w_products(c):
                    w_part[slot, w_rows] += dot_nt(x_buf[:, rows_of(c)], chunk_of(c))

                over_chunks(w_products)
                swap = to_mate(w_part.at[slot, w_rows], w_other.at[slot, w_rows], swap_send.at[0, slot], swap_recv.at[0, slot])
                swap.start()
                g_swap.wait()
                t_rows = buf2[z, pl.ds(y, 2), :, TILES[2]].reshape(BLOCK, TILE)
                t_mat = merged(t_rows, group, g_part[slot] + g_other[slot])
                run_middle()
                swap.wait()
                y_t = dot_nt(w_part[slot, w_rows] + w_other[slot, w_rows], t_mat)

            def update(c):
                x_buf[:, rows_of(c)] -= dot_nn(y_t, chunk_of(c))

            over_chunks(update)
            return carry

        lax.fori_loop(0, 8, block_step, 0)

    act = functools.partial
    apply_group(2, {1: [act(advance, 0, 0)], 2: [act(advance, 1, 1)], 6: [act(forward, 0, 1)]}, {})
    forward(1, 2)
    advance(0, 1)
    finish(1, 2)
    apply_group(1, {}, {
        3: [act(forward, 0, 2, 3), act(begin, 0, 2, 1)],
        4: [act(forward, 0, 2), act(forward, 0, 2, 2), act(begin, 0, 2, 0)],
        7: [act(forward, 0, 2, 1)],
    })
    finish(0, 2)
    finish(0, 2, 3)
    apply_group(0, {2: [act(finish, 0, 2, 2)], 4: [act(finish, 0, 2, 1)], 6: [act(finish, 0, 2, 0)]},
                {0: [act(forward, 0, 2, 0)]})
    out_ref[...] = x_buf[...]

    give.wait_send()
    swap_line.wait_send()
    give_half.wait_send()
    for kind in range(3):
        for copy in line_copies(kind, False):
            copy.wait_send()
    for key in message_keys():
        for copy in messages(*key, False):
            copy.wait_send()


def solution(mesh):
    def local_apply(v_loc, t_loc, z_loc):
        groups, width = t_loc.shape[0], t_loc.shape[1]
        local_rows = v_loc.shape[0]
        cols = 2 * z_loc.shape[1]
        t_tile = jnp.pad(t_loc.transpose(1, 0, 2).reshape(width, groups * width), ((0, 0), (0, TILE - groups * width)))
        any_spec = pl.BlockSpec(memory_space=pl.ANY)
        dma = pltpu.SemaphoreType.DMA

        def vmem(*shape):
            return pltpu.VMEM(shape, jnp.float32)

        x_t = pl.pallas_call(
            kernel,
            out_shape=jax.ShapeDtypeStruct((cols, local_rows), jnp.float32),
            in_specs=[any_spec, any_spec, any_spec],
            out_specs=pl.BlockSpec(memory_space=pltpu.VMEM),
            scratch_shapes=[
                *(vmem(SIDE, SIDE, SIDE, TILES[group] + EXTRA[group], WIDTH, TILE) for group in (2, 1, 0)),
                vmem(cols, local_rows),
                vmem(2, cols + HALF, BLOCK), vmem(2, cols + HALF, BLOCK),
                vmem(2, BLOCK, BLOCK), vmem(2, BLOCK, BLOCK),
                vmem(SIDE, WIDTH, QUARTER), vmem(SIDE, WIDTH, TILE),
                vmem(HALF, HALF), vmem(HALF, HALF), vmem(SIDE, HALF // 2, HALF), vmem(HALF, HALF), vmem(HALF, HALF),
                dma((3,)), dma((3,)), dma((len(TABLE),)), dma((len(TABLE),)), dma((2, 2)), dma((2, 2)),
                dma((4, 3)), dma((4, 3)), dma((2,)),
            ],
            compiler_params=pltpu.CompilerParams(collective_id=0, has_side_effects=True, vmem_limit_bytes=67043328),
        )(v_loc.T, t_tile, z_loc.T)
        return x_t.T

    return jax.shard_map(local_apply, mesh=mesh,
                         in_specs=(P('row', 'col'), P('col', None, None), P(None, ('col', 'row'))),
                         out_specs=P('row', 'col'), check_vma=False)
```

```python
import jax
import jax.numpy as jnp
from jax import lax
from jax.experimental import pallas as pl
from jax.experimental.pallas import tpu as pltpu
from jax.sharding import PartitionSpec as P

HIGHEST = lax.Precision.HIGHEST
MESH = pl.DeviceIdType.MESH
BLOCK = 256
HALF = BLOCK // 2
TILE = 128
SIDE = 4
WIDTH = 32
TILES = {2: 8, 1: 16, 0: 24}
EXTRA = {2: 1, 1: 0, 0: 0}
OWNERS = (1, 0)
ROUND_T = 3
QUARTERS = {group: TILES[group] // SIDE * TILE for group in OWNERS}
ORDERS = ((2, 1, 0), (1, 0, 2), (0, 2, 1))
RANGES = {
    2: ((7, 9), (0, 3), (3, 7)),
    1: ((12, 16), (0, 7), (7, 12)),
    0: ((18, 24), (0, 10), (10, 18)),
    3: ((0, 0), (0, 1), (1, 2)),
}
ROUNDS = (2, 1, 0, ROUND_T)
PRELUDE = (
    'L1 f20 f10 L2', 'f00 e20 b21 e10', 'b11 L3 e00 L4', 'b30 f21 f11 f30', 'e21 b22 b223 b222',
    'b221 f223 e11 e30', 'b31 f222 f22 b220', 'f221 e223 b12 f31', 'b01 e222 f220 e22',
)
EVENTS = {
    (2, 'before'): {3: 'e220', 5: 'f122', 6: 'e123', 7: 'f32'},
    (2, 'mid'): {0: 'e221', 1: 'b123', 2: 'f12', 3: 'b122 f123', 4: 'e31', 5: 'b32 f01', 6: 'e122', 7: 'b121'},
    (1, 'before'): {0: 'e32 e12', 2: 'f120', 5: 'f02 f023'},
    (1, 'mid'): {0: 'b120 f121', 1: 'e01 b02', 3: 'e121 b023', 4: 'e120', 5: 'b022', 6: 'e023', 7: 'f022'},
    (0, 'before'): {0: 'b021 e022 b020 f021 e02', 4: 'e021', 6: 'e020'},
    (0, 'mid'): {1: 'f020'},
}


def dot_nn(a, b):
    return lax.dot_general(a, b, (((1,), (0,)), ((), ())), precision=HIGHEST, preferred_element_type=jnp.float32)


def dot_nt(a, b):
    return lax.dot_general(a, b, (((1,), (1,)), ((), ())), precision=HIGHEST, preferred_element_type=jnp.float32)


def regions(group, part, phase, plane, coords, pos, half):
    order = ORDERS[part]
    low, high = RANGES[group][part]
    index = list(coords)
    index[order[phase]] = pos
    for axis in order[:phase]:
        index[axis] = pl.ds(0, SIDE)
    if phase == 0:
        middle = (low + high + 1) // 2
        low, high = ((low, middle), (middle, high))[half]
    else:
        index[order[1 if plane is not None and order[0] == 0 else 0]] = pl.ds(2 * half, 2)
    if plane is not None:
        index[0] = plane
        low = max(low, 2 * plane)
    return (*index, pl.ds(low, high - low)) if low < high else None


def planes_of(group, phase):
    return (None, 3, 2, 1, 0) if phase == 2 and group != ROUND_T else (None,)


def parts_of(group, phase, plane):
    if planes_of(group, phase) == (None,):
        return (0, 1, 2)
    return (0,) if plane is None else (1, 2)


def message_keys():
    for group in ROUNDS:
        for phase in range(3):
            for plane in planes_of(group, phase):
                for piece in range(3):
                    yield group, phase, plane, piece


def half_of(piece, way):
    return 1 - way if piece == 1 else way


def semaphore_table():
    table = {}
    for group, phase, plane, piece in message_keys():
        for part in parts_of(group, phase, plane):
            for way in range(2):
                if regions(group, part, phase, plane, (0, 0, 0), 0, half_of(piece, way)) is not None:
                    table[group, phase, plane, piece, part, way] = len(table)
    return table


TABLE = semaphore_table()


def kernel(v_hbm, t_hbm, z_hbm, out_ref, buf2, buf1, buf0, buf_t, x_buf, w_part, w_other, g_part, g_other, quarters_1,
           quarters_0, t_line,
           line_part, line_other, line_half, line_gram, line_t,
           load_sem, x_sem, send_sem, recv_sem, swap_send, swap_recv, line_send, line_recv, line_load):
    bufs = {2: buf2, 1: buf1, 0: buf0, ROUND_T: buf_t}
    quarters = {1: quarters_1, 0: quarters_0}
    cols, local_rows = x_buf.shape
    share = cols // 2
    me = lax.axis_index('row')
    mate = 1 - me
    chip = lax.axis_index('col')
    coords = (chip // (SIDE * SIDE), lax.rem(chip // SIDE, SIDE), lax.rem(chip, SIDE))
    strides = (SIDE * SIDE, SIDE, 1)
    my_x = coords[2]

    def shifted(axis, by):
        return lax.rem(coords[axis] + by + SIDE, SIDE)

    def neighbour(axis, by):
        return {'col': chip + (shifted(axis, by) - coords[axis]) * strides[axis]}

    def to_mate(src, dst, send, recv):
        return pltpu.make_async_remote_copy(src_ref=src, dst_ref=dst, send_sem=send, recv_sem=recv,
                                            device_id={'row': mate}, device_id_type=MESH)

    for group in TILES:
        for z in range(1, SIDE):
            shape = (SIDE, SIDE, 2 * z, WIDTH, TILE)
            bufs[group][z, :, :, 0:2 * z, :, :] = jnp.zeros(shape, jnp.float32)

    barrier = pltpu.get_barrier_semaphore()
    pl.semaphore_signal(barrier, inc=1, device_id={'row': mate}, device_id_type=MESH)
    for axis, by in ((0, 1), (0, -1), (1, 1), (1, -1), (2, 1), (2, 2), (2, 3)):
        pl.semaphore_signal(barrier, inc=1, device_id=neighbour(axis, by), device_id_type=MESH)
    pl.semaphore_wait(barrier, 8)

    own = {group: bufs[group].at[coords[0], coords[1], coords[2]] for group in TILES}

    def load(group):
        first = local_rows - TILES[group] * TILE
        for tile in range(TILES[group]):
            src = v_hbm.at[pl.ds(group * WIDTH, WIDTH), pl.ds(first + tile * TILE, TILE)]
            pltpu.make_async_copy(src, own[group].at[tile], load_sem.at[group]).start()
        if group == 2:
            pltpu.make_async_copy(t_hbm, own[2].at[TILES[2]], load_sem.at[2]).start()

    def loaded(group):
        tiles = pl.ds(0, TILES[group] + (1 if group == 2 else 0))
        pltpu.make_async_copy(own[group].at[tiles], own[group].at[tiles], load_sem.at[group]).wait()

    mine = pl.ds(pl.multiple_of(me * local_rows, TILE), local_rows)
    theirs = pl.ds(pl.multiple_of(mate * local_rows, TILE), local_rows)
    my_cols = x_buf.at[pl.ds(pl.multiple_of(me * share, 8), share), :]
    their_cols = x_buf.at[pl.ds(pl.multiple_of(mate * share, 8), share), :]
    keep = pltpu.make_async_copy(z_hbm.at[:, mine], my_cols, x_sem.at[0])
    give = to_mate(z_hbm.at[:, theirs], my_cols, x_sem.at[1], x_sem.at[2])
    take = to_mate(z_hbm.at[:, theirs], their_cols, x_sem.at[1], x_sem.at[2])

    def messages(group, phase, plane, piece, incoming):
        copies = []
        for part in parts_of(group, phase, plane):
            axis = ORDERS[part][phase]
            for way in range(2):
                sign = 1 - 2 * way
                pos = shifted(axis, (-sign if piece == 2 else 0) + (-sign if incoming else 0))
                index = regions(group, part, phase, plane, coords, pos, half_of(piece, way))
                if index is None:
                    continue
                number = TABLE[group, phase, plane, piece, part, way]
                ref = bufs[group].at[index]
                copies.append(pltpu.make_async_remote_copy(
                    src_ref=ref, dst_ref=ref, send_sem=send_sem.at[number], recv_sem=recv_sem.at[number],
                    device_id=neighbour(axis, sign), device_id_type=MESH))
        return copies

    def begin(group, phase, plane=None):
        for piece in range(2):
            for copy in messages(group, phase, plane, piece, False):
                copy.start()

    def forward(group, phase, plane=None):
        for copy in messages(group, phase, plane, 0, True):
            copy.wait_recv()
        for copy in messages(group, phase, plane, 2, False):
            copy.start()

    def finish(group, phase, plane=None):
        for piece in range(1, 3):
            for copy in messages(group, phase, plane, piece, True):
                copy.wait_recv()

    def quarter(group, x):
        first = local_rows - TILES[group] * TILE
        lanes = pl.ds(pl.multiple_of(first + x * QUARTERS[group], TILE), QUARTERS[group])
        return v_hbm.at[pl.ds(group * WIDTH, WIDTH), lanes]

    def line_copies(kind, incoming):
        copies = []
        for by in range(1, SIDE):
            other = shifted(2, by)
            slot = shifted(2, -by) if incoming else my_x
            if kind < 2:
                src, dst = quarter(OWNERS[kind], other), quarters[OWNERS[kind]].at[slot]
            elif kind == 2:
                src, dst = t_hbm, t_line.at[slot]
            else:
                src, dst = line_half.at[my_x], line_half.at[slot]
            copies.append(pltpu.make_async_remote_copy(
                src_ref=src, dst_ref=dst, send_sem=line_send.at[kind, by - 1], recv_sem=line_recv.at[kind, by - 1],
                device_id=neighbour(2, by), device_id_type=MESH))
        return copies

    own_copies = [pltpu.make_async_copy(quarter(group, my_x), quarters[group].at[my_x], line_load.at[i])
                  for i, group in enumerate(OWNERS)]
    own_copies.append(pltpu.make_async_copy(t_hbm, t_line.at[my_x], line_load.at[2]))
    swap_line = to_mate(line_part, line_other, line_send.at[4, 0], line_recv.at[4, 0])
    my_half = pl.ds(pl.multiple_of(me * (HALF // 2), 8), HALF // 2)
    their_half = pl.ds(pl.multiple_of(mate * (HALF // 2), 8), HALF // 2)
    give_half = to_mate(line_gram.at[:, my_half], line_gram.at[:, my_half], line_send.at[4, 1], line_recv.at[4, 1])
    take_half = to_mate(line_gram.at[:, my_half], line_gram.at[:, their_half], line_send.at[4, 1], line_recv.at[4, 1])

    def block_diagonal(t_rows, group):
        size = t_rows.shape[0]
        column = t_rows[:, group * WIDTH:(group + 1) * WIDTH]
        wide = jnp.concatenate([column] * (size // WIDTH), axis=1)
        row_id = lax.broadcasted_iota(jnp.int32, (size, size), 0)
        col_id = lax.broadcasted_iota(jnp.int32, (size, size), 1)
        return jnp.where(row_id // WIDTH == col_id // WIDTH, wide, 0.0), row_id, col_id

    def merged(t_rows, group, gram):
        t_mat, row_id, col_id = block_diagonal(t_rows, group)
        size = WIDTH
        while size < gram.shape[0]:
            pick = (row_id // size + 1 == col_id // size) & (row_id // (2 * size) == col_id // (2 * size))
            t_mat = t_mat - dot_nn(dot_nn(t_mat, jnp.where(pick, gram, 0.0)), t_mat)
            size *= 2
        return t_mat

    def line_1():
        for kind in range(3):
            for copy in line_copies(kind, True):
                copy.wait_recv()
        for copy in own_copies:
            copy.wait()
        for i, group in enumerate(OWNERS):
            rows = quarters[group][...].reshape(HALF, QUARTERS[group])
            line_part[i] = dot_nt(rows, rows)
        swap_line.start()

    def line_2():
        swap_line.wait_recv()
        line_half[my_x] = line_part[:, my_half] + line_other[:, my_half]
        for copy in line_copies(3, False):
            copy.start()

    def line_3():
        for copy in line_copies(3, True):
            copy.wait_recv()
        line_gram[:, my_half] = (line_half[0] + line_half[1]) + (line_half[2] + line_half[3])
        give_half.start()

    def line_4():
        take_half.wait_recv()
        mine = pl.ds(pl.multiple_of(my_x * WIDTH, 8), WIDTH)
        for i, group in enumerate(OWNERS):
            line_t[i] = merged(t_line[...].reshape(HALF, TILE), group, line_gram[i])
            buf_t[coords[0], coords[1], coords[2], i] = line_t[i, mine]

    actions = {'b': begin, 'f': forward, 'e': finish}
    lines = {'L1': line_1, 'L2': line_2, 'L3': line_3, 'L4': line_4}

    def act(events):
        for event in events.split():
            if event in lines:
                lines[event]()
            else:
                actions[event[0]](*(int(digit) for digit in event[1:]))

    load(2)
    for kind in range(3):
        for copy in line_copies(kind, False):
            copy.start()
    for copy in own_copies:
        copy.start()
    load(1)
    load(0)
    loaded(2)
    begin(2, 0)
    loaded(1)
    begin(1, 0)
    loaded(0)
    begin(0, 0)
    keep.start()
    give.start()
    for events in PRELUDE:
        act(events)
    keep.wait()
    take.wait_recv()

    def apply_group(group):
        buf = bufs[group]
        tiles = TILES[group]
        first_row = local_rows - tiles * TILE

        def block_step(step, carry):
            blk = 7 - step
            z, y = blk // 2, 2 * lax.rem(blk, 2)
            slot = lax.rem(step, 2)

            def run(where):
                for when, events in EVENTS.get((group, where), {}).items():
                    @pl.when(step == when)
                    def _():
                        act(events)

            def block_of(tile, count):
                pieces = [buf[z, pl.ds(y, 2), :, tile + i].reshape(BLOCK, TILE) for i in range(count)]
                return jnp.concatenate(pieces, axis=1)

            def rows_of(tile, count):
                return pl.ds(pl.multiple_of(first_row + tile * TILE, TILE), count * TILE)

            def over_rows(body):
                @pl.when(blk >= 4)
                def _():
                    body(4, 4)

                lax.fori_loop(blk // 4, tiles // 8, lambda c, carry: (body(8 * c, 8), carry)[1], 0)

            run('before')
            if group in OWNERS:
                w_part[slot] = jnp.zeros(w_part.shape[1:], jnp.float32)

                def products(tile, count):
                    v_c = block_of(tile, count)
                    x_c = x_buf[:, rows_of(tile, count)]
                    w_part[slot] += dot_nt(jnp.concatenate([x_c, v_c[:HALF]], axis=0), v_c)

                over_rows(products)
                swap = to_mate(w_part.at[slot], w_other.at[slot], swap_send.at[0, slot], swap_recv.at[0, slot])
                swap.start()
                run('mid')
                swap.wait()
                total = w_part[slot] + w_other[slot]
                w_t, cross = total[:cols], total[cols:, HALF:]
                i = OWNERS.index(group)
                t_1 = buf_t[z, y, :, i].reshape(HALF, HALF)
                t_2 = buf_t[z, y + 1, :, i].reshape(HALF, HALF)
            else:
                g_part[slot] = jnp.zeros(g_part.shape[1:], jnp.float32)

                def gram_products(tile, count):
                    v_c = block_of(tile, count)
                    g_part[slot] += dot_nt(v_c, v_c)

                over_rows(gram_products)
                g_swap = to_mate(g_part.at[slot], g_other.at[slot], swap_send.at[1, slot], swap_recv.at[1, slot])
                g_swap.start()
                w_rows = pl.ds(0, cols)
                w_part[slot, w_rows] = jnp.zeros((cols, BLOCK), jnp.float32)

                def w_products(tile, count):
                    w_part[slot, w_rows] += dot_nt(x_buf[:, rows_of(tile, count)], block_of(tile, count))

                over_rows(w_products)
                swap = to_mate(w_part.at[slot, w_rows], w_other.at[slot, w_rows], swap_send.at[0, slot], swap_recv.at[0, slot])
                swap.start()
                g_swap.wait()
                gram = g_part[slot] + g_other[slot]
                t_rows = buf[z, pl.ds(y, 2), :, tiles].reshape(BLOCK, TILE)
                t_1 = merged(t_rows[:HALF], group, gram[:HALF, :HALF])
                t_2 = merged(t_rows[HALF:], group, gram[HALF:, HALF:])
                cross = gram[:HALF, HALF:]
                run('mid')
                swap.wait()
                w_t = w_part[slot, w_rows] + w_other[slot, w_rows]

            y_2 = dot_nt(w_t[:, HALF:], t_2)
            y_1 = dot_nt(w_t[:, :HALF] - dot_nt(y_2, cross), t_1)
            y_t = jnp.concatenate([y_1, y_2], axis=1)

            def update(tile, count):
                x_buf[:, rows_of(tile, count)] -= dot_nn(y_t, block_of(tile, count))

            over_rows(update)
            return carry

        lax.fori_loop(0, 8, block_step, 0)

    apply_group(2)
    apply_group(1)
    apply_group(0)
    out_ref[...] = x_buf[...]

    give.wait_send()
    swap_line.wait_send()
    give_half.wait_send()
    for kind in range(4):
        for copy in line_copies(kind, False):
            copy.wait_send()
    for key in message_keys():
        for copy in messages(*key, False):
            copy.wait_send()


def solution(mesh):
    def local_apply(v_loc, t_loc, z_loc):
        groups, width = t_loc.shape[0], t_loc.shape[1]
        local_rows = v_loc.shape[0]
        cols = 2 * z_loc.shape[1]
        t_tile = jnp.pad(t_loc.transpose(1, 0, 2).reshape(width, groups * width), ((0, 0), (0, TILE - groups * width)))
        any_spec = pl.BlockSpec(memory_space=pl.ANY)
        dma = pltpu.SemaphoreType.DMA

        def vmem(*shape):
            return pltpu.VMEM(shape, jnp.float32)

        x_t = pl.pallas_call(
            kernel,
            out_shape=jax.ShapeDtypeStruct((cols, local_rows), jnp.float32),
            in_specs=[any_spec, any_spec, any_spec],
            out_specs=pl.BlockSpec(memory_space=pltpu.VMEM),
            scratch_shapes=[
                *(vmem(SIDE, SIDE, SIDE, TILES[group] + EXTRA[group], WIDTH, TILE) for group in (2, 1, 0)),
                vmem(SIDE, SIDE, SIDE, len(OWNERS), WIDTH, TILE),
                vmem(cols, local_rows),
                vmem(2, cols + HALF, BLOCK), vmem(2, cols + HALF, BLOCK),
                vmem(2, BLOCK, BLOCK), vmem(2, BLOCK, BLOCK),
                *(vmem(SIDE, WIDTH, QUARTERS[group]) for group in OWNERS), vmem(SIDE, WIDTH, TILE),
                vmem(2, HALF, HALF), vmem(2, HALF, HALF), vmem(SIDE, 2, HALF // 2, HALF),
                vmem(2, HALF, HALF), vmem(2, HALF, HALF),
                dma((3,)), dma((3,)), dma((len(TABLE),)), dma((len(TABLE),)), dma((2, 2)), dma((2, 2)),
                dma((5, 3)), dma((5, 3)), dma((3,)),
            ],
            compiler_params=pltpu.CompilerParams(collective_id=0, has_side_effects=True, vmem_limit_bytes=67043328),
        )(v_loc.T, t_tile, z_loc.T)
        return x_t.T

    return jax.shard_map(local_apply, mesh=mesh,
                         in_specs=(P('row', 'col'), P('col', None, None), P(None, ('col', 'row'))),
                         out_specs=P('row', 'col'), check_vma=False)
```

```python
import jax
import jax.numpy as jnp
from jax import lax
from jax.experimental import pallas as pl
from jax.experimental.pallas import tpu as pltpu
from jax.sharding import PartitionSpec as P

HIGHEST = lax.Precision.HIGHEST
MESH = pl.DeviceIdType.MESH
BLOCK = 256
HALF = BLOCK // 2
TILE = 128
SIDE = 4
WIDTH = 32
TILES = {2: 8, 1: 16, 0: 24}
EXTRA = {2: 1, 1: 0, 0: 0}
OWNERS = (1, 0)
ROUND_T = 3
QUARTERS = {group: TILES[group] // SIDE * TILE for group in OWNERS}
ORDERS = ((2, 1, 0), (1, 0, 2), (0, 2, 1))
RANGES = {
    2: ((7, 9), (0, 3), (3, 7)),
    1: ((12, 16), (0, 7), (7, 12)),
    0: ((18, 24), (0, 10), (10, 18)),
    3: ((0, 0), (0, 1), (1, 2)),
}
ROUNDS = (2, 1, 0, ROUND_T)
PRELUDE = (
    'L1 f20 f10 L2', 'f00 e20 b21 e10', 'b11 L3 e00 L4', 'b30 f21 f11 f30', 'e21 b22 b223 b222',
    'b221 f223 e11 e30', 'b31 f222 f22 b220', 'f221 e223 b12 f31', 'b01 e222 f220 e22',
)
EVENTS = {
    (2, 'before'): {3: 'e220', 5: 'f122', 6: 'e123'},
    (2, 'mid'): {0: 'e221', 1: 'e31 b32 b123', 2: 'f12', 3: 'b122 f123', 4: 'f32', 5: 'f01', 6: 'e122', 7: 'b121'},
    (1, 'before'): {0: 'e32 e12', 2: 'f120', 5: 'f02 f023'},
    (1, 'mid'): {0: 'b120 f121', 1: 'e01 b02', 3: 'e121 b023', 4: 'e120', 5: 'b022', 6: 'e023 b021', 7: 'f022'},
    (0, 'before'): {0: 'e02', 2: 'e022', 4: 'e021', 6: 'e020'},
    (0, 'mid'): {0: 'f021 b020', 2: 'f020'},
}


def dot_nn(a, b):
    return lax.dot_general(a, b, (((1,), (0,)), ((), ())), precision=HIGHEST, preferred_element_type=jnp.float32)


def dot_nt(a, b):
    return lax.dot_general(a, b, (((1,), (1,)), ((), ())), precision=HIGHEST, preferred_element_type=jnp.float32)


def regions(group, part, phase, plane, coords, pos, half):
    order = ORDERS[part]
    low, high = RANGES[group][part]
    index = list(coords)
    index[order[phase]] = pos
    for axis in order[:phase]:
        index[axis] = pl.ds(0, SIDE)
    if phase == 0:
        middle = (low + high + 1) // 2
        low, high = ((low, middle), (middle, high))[half]
    else:
        index[order[1 if plane is not None and order[0] == 0 else 0]] = pl.ds(2 * half, 2)
    if plane is not None:
        index[0] = plane
        low = max(low, 2 * plane)
    return (*index, pl.ds(low, high - low)) if low < high else None


def planes_of(group, phase):
    return (None, 3, 2, 1, 0) if phase == 2 and group != ROUND_T else (None,)


def parts_of(group, phase, plane):
    if planes_of(group, phase) == (None,):
        return (0, 1, 2)
    return (0,) if plane is None else (1, 2)


def message_keys():
    for group in ROUNDS:
        for phase in range(3):
            for plane in planes_of(group, phase):
                for piece in range(3):
                    yield group, phase, plane, piece


def half_of(piece, way):
    return 1 - way if piece == 1 else way


def semaphore_table():
    table = {}
    for group, phase, plane, piece in message_keys():
        for part in parts_of(group, phase, plane):
            for way in range(2):
                if regions(group, part, phase, plane, (0, 0, 0), 0, half_of(piece, way)) is not None:
                    table[group, phase, plane, piece, part, way] = len(table)
    return table


TABLE = semaphore_table()


def kernel(v_hbm, t_hbm, z_hbm, out_ref, buf2, buf1, buf0, buf_t, x_buf, w_part, w_other, g_part, g_other, quarters_1,
           quarters_0, t_line,
           line_part, line_other, line_half, line_gram, line_t,
           load_sem, x_sem, send_sem, recv_sem, swap_send, swap_recv, line_send, line_recv, line_load):
    bufs = {2: buf2, 1: buf1, 0: buf0, ROUND_T: buf_t}
    quarters = {1: quarters_1, 0: quarters_0}
    cols, local_rows = x_buf.shape
    share = cols // 2
    me = lax.axis_index('row')
    mate = 1 - me
    chip = lax.axis_index('col')
    coords = (chip // (SIDE * SIDE), lax.rem(chip // SIDE, SIDE), lax.rem(chip, SIDE))
    strides = (SIDE * SIDE, SIDE, 1)
    my_x = coords[2]

    def shifted(axis, by):
        return lax.rem(coords[axis] + by + SIDE, SIDE)

    def neighbour(axis, by):
        return {'col': chip + (shifted(axis, by) - coords[axis]) * strides[axis]}

    def to_mate(src, dst, send, recv):
        return pltpu.make_async_remote_copy(src_ref=src, dst_ref=dst, send_sem=send, recv_sem=recv,
                                            device_id={'row': mate}, device_id_type=MESH)

    for group in TILES:
        for z in range(1, SIDE):
            shape = (SIDE, SIDE, 2 * z, WIDTH, TILE)
            bufs[group][z, :, :, 0:2 * z, :, :] = jnp.zeros(shape, jnp.float32)

    barrier = pltpu.get_barrier_semaphore()
    pl.semaphore_signal(barrier, inc=1, device_id={'row': mate}, device_id_type=MESH)
    for axis, by in ((0, 1), (0, -1), (1, 1), (1, -1), (2, 1), (2, 2), (2, 3)):
        pl.semaphore_signal(barrier, inc=1, device_id=neighbour(axis, by), device_id_type=MESH)
    pl.semaphore_wait(barrier, 8)

    own = {group: bufs[group].at[coords[0], coords[1], coords[2]] for group in TILES}

    def load(group):
        first = local_rows - TILES[group] * TILE
        for tile in range(TILES[group]):
            src = v_hbm.at[pl.ds(group * WIDTH, WIDTH), pl.ds(first + tile * TILE, TILE)]
            pltpu.make_async_copy(src, own[group].at[tile], load_sem.at[group]).start()
        if group == 2:
            pltpu.make_async_copy(t_hbm, own[2].at[TILES[2]], load_sem.at[2]).start()

    def loaded(group):
        tiles = pl.ds(0, TILES[group] + (1 if group == 2 else 0))
        pltpu.make_async_copy(own[group].at[tiles], own[group].at[tiles], load_sem.at[group]).wait()

    mine = pl.ds(pl.multiple_of(me * local_rows, TILE), local_rows)
    theirs = pl.ds(pl.multiple_of(mate * local_rows, TILE), local_rows)
    my_cols = x_buf.at[pl.ds(pl.multiple_of(me * share, 8), share), :]
    their_cols = x_buf.at[pl.ds(pl.multiple_of(mate * share, 8), share), :]
    keep = pltpu.make_async_copy(z_hbm.at[:, mine], my_cols, x_sem.at[0])
    give = to_mate(z_hbm.at[:, theirs], my_cols, x_sem.at[1], x_sem.at[2])
    take = to_mate(z_hbm.at[:, theirs], their_cols, x_sem.at[1], x_sem.at[2])

    def messages(group, phase, plane, piece, incoming):
        copies = []
        for part in parts_of(group, phase, plane):
            axis = ORDERS[part][phase]
            for way in range(2):
                sign = 1 - 2 * way
                pos = shifted(axis, (-sign if piece == 2 else 0) + (-sign if incoming else 0))
                index = regions(group, part, phase, plane, coords, pos, half_of(piece, way))
                if index is None:
                    continue
                number = TABLE[group, phase, plane, piece, part, way]
                ref = bufs[group].at[index]
                copies.append(pltpu.make_async_remote_copy(
                    src_ref=ref, dst_ref=ref, send_sem=send_sem.at[number], recv_sem=recv_sem.at[number],
                    device_id=neighbour(axis, sign), device_id_type=MESH))
        return copies

    def begin(group, phase, plane=None):
        for piece in range(2):
            for copy in messages(group, phase, plane, piece, False):
                copy.start()

    def forward(group, phase, plane=None):
        for copy in messages(group, phase, plane, 0, True):
            copy.wait_recv()
        for copy in messages(group, phase, plane, 2, False):
            copy.start()

    def finish(group, phase, plane=None):
        for piece in range(1, 3):
            for copy in messages(group, phase, plane, piece, True):
                copy.wait_recv()

    def quarter(group, x):
        first = local_rows - TILES[group] * TILE
        lanes = pl.ds(pl.multiple_of(first + x * QUARTERS[group], TILE), QUARTERS[group])
        return v_hbm.at[pl.ds(group * WIDTH, WIDTH), lanes]

    def line_copies(kind, incoming):
        copies = []
        for by in range(1, SIDE):
            other = shifted(2, by)
            slot = shifted(2, -by) if incoming else my_x
            if kind < 2:
                src, dst = quarter(OWNERS[kind], other), quarters[OWNERS[kind]].at[slot]
            elif kind == 2:
                src, dst = t_hbm, t_line.at[slot]
            else:
                src, dst = line_half.at[my_x], line_half.at[slot]
            copies.append(pltpu.make_async_remote_copy(
                src_ref=src, dst_ref=dst, send_sem=line_send.at[kind, by - 1], recv_sem=line_recv.at[kind, by - 1],
                device_id=neighbour(2, by), device_id_type=MESH))
        return copies

    own_copies = [pltpu.make_async_copy(quarter(group, my_x), quarters[group].at[my_x], line_load.at[i])
                  for i, group in enumerate(OWNERS)]
    own_copies.append(pltpu.make_async_copy(t_hbm, t_line.at[my_x], line_load.at[2]))
    swap_line = to_mate(line_part, line_other, line_send.at[4, 0], line_recv.at[4, 0])
    my_half = pl.ds(pl.multiple_of(me * (HALF // 2), 8), HALF // 2)
    their_half = pl.ds(pl.multiple_of(mate * (HALF // 2), 8), HALF // 2)
    give_half = to_mate(line_gram.at[:, my_half], line_gram.at[:, my_half], line_send.at[4, 1], line_recv.at[4, 1])
    take_half = to_mate(line_gram.at[:, my_half], line_gram.at[:, their_half], line_send.at[4, 1], line_recv.at[4, 1])

    def block_diagonal(t_rows, group):
        size = t_rows.shape[0]
        column = t_rows[:, group * WIDTH:(group + 1) * WIDTH]
        wide = jnp.concatenate([column] * (size // WIDTH), axis=1)
        row_id = lax.broadcasted_iota(jnp.int32, (size, size), 0)
        col_id = lax.broadcasted_iota(jnp.int32, (size, size), 1)
        return jnp.where(row_id // WIDTH == col_id // WIDTH, wide, 0.0), row_id, col_id

    def merged(t_rows, group, gram):
        t_mat, row_id, col_id = block_diagonal(t_rows, group)
        size = WIDTH
        while size < gram.shape[0]:
            pick = (row_id // size + 1 == col_id // size) & (row_id // (2 * size) == col_id // (2 * size))
            t_mat = t_mat - dot_nn(dot_nn(t_mat, jnp.where(pick, gram, 0.0)), t_mat)
            size *= 2
        return t_mat

    def line_1():
        for kind in range(3):
            for copy in line_copies(kind, True):
                copy.wait_recv()
        for copy in own_copies:
            copy.wait()
        for i, group in enumerate(OWNERS):
            rows = quarters[group][...].reshape(HALF, QUARTERS[group])
            line_part[i] = dot_nt(rows, rows)
        swap_line.start()

    def line_2():
        swap_line.wait_recv()
        line_half[my_x] = line_part[:, my_half] + line_other[:, my_half]
        for copy in line_copies(3, False):
            copy.start()

    def line_3():
        for copy in line_copies(3, True):
            copy.wait_recv()
        line_gram[:, my_half] = (line_half[0] + line_half[1]) + (line_half[2] + line_half[3])
        give_half.start()

    def line_4():
        take_half.wait_recv()
        mine = pl.ds(pl.multiple_of(my_x * WIDTH, 8), WIDTH)
        for i, group in enumerate(OWNERS):
            line_t[i] = merged(t_line[...].reshape(HALF, TILE), group, line_gram[i])
            buf_t[coords[0], coords[1], coords[2], i] = line_t[i, mine]

    actions = {'b': begin, 'f': forward, 'e': finish}
    lines = {'L1': line_1, 'L2': line_2, 'L3': line_3, 'L4': line_4}

    def act(events):
        for event in events.split():
            if event in lines:
                lines[event]()
            else:
                actions[event[0]](*(int(digit) for digit in event[1:]))

    load(2)
    for kind in range(3):
        for copy in line_copies(kind, False):
            copy.start()
    for copy in own_copies:
        copy.start()
    load(1)
    load(0)
    loaded(2)
    begin(2, 0)
    loaded(1)
    begin(1, 0)
    loaded(0)
    begin(0, 0)
    keep.start()
    give.start()
    for events in PRELUDE:
        act(events)
    keep.wait()
    take.wait_recv()

    def apply_group(group):
        buf = bufs[group]
        tiles = TILES[group]
        first_row = local_rows - tiles * TILE

        def block_step(step, carry):
            blk = 7 - step
            z, y = blk // 2, 2 * lax.rem(blk, 2)
            slot = lax.rem(step, 2)

            def run(where):
                for when, events in EVENTS.get((group, where), {}).items():
                    @pl.when(step == when)
                    def _():
                        act(events)

            def block_of(tile, count):
                pieces = [buf[z, pl.ds(y, 2), :, tile + i].reshape(BLOCK, TILE) for i in range(count)]
                return jnp.concatenate(pieces, axis=1)

            def rows_of(tile, count):
                return pl.ds(pl.multiple_of(first_row + tile * TILE, TILE), count * TILE)

            def over_rows(body):
                @pl.when(blk >= 4)
                def _():
                    body(4, 4)

                lax.fori_loop(blk // 4, tiles // 8, lambda c, carry: (body(8 * c, 8), carry)[1], 0)

            run('before')
            if group in OWNERS:
                w_part[slot] = jnp.zeros(w_part.shape[1:], jnp.float32)

                def products(tile, count):
                    v_c = block_of(tile, count)
                    x_c = x_buf[:, rows_of(tile, count)]
                    w_part[slot] += dot_nt(jnp.concatenate([x_c, v_c[:HALF]], axis=0), v_c)

                over_rows(products)
                swap = to_mate(w_part.at[slot], w_other.at[slot], swap_send.at[0, slot], swap_recv.at[0, slot])
                swap.start()
                run('mid')
                swap.wait()
                total = w_part[slot] + w_other[slot]
                w_t, cross = total[:cols], total[cols:, HALF:]
                i = OWNERS.index(group)
                t_1 = buf_t[z, y, :, i].reshape(HALF, HALF)
                t_2 = buf_t[z, y + 1, :, i].reshape(HALF, HALF)
            else:
                g_part[slot] = jnp.zeros(g_part.shape[1:], jnp.float32)

                def gram_products(tile, count):
                    v_c = block_of(tile, count)
                    g_part[slot] += dot_nt(v_c, v_c)

                over_rows(gram_products)
                g_swap = to_mate(g_part.at[slot], g_other.at[slot], swap_send.at[1, slot], swap_recv.at[1, slot])
                g_swap.start()
                w_rows = pl.ds(0, cols)
                w_part[slot, w_rows] = jnp.zeros((cols, BLOCK), jnp.float32)

                def w_products(tile, count):
                    w_part[slot, w_rows] += dot_nt(x_buf[:, rows_of(tile, count)], block_of(tile, count))

                over_rows(w_products)
                swap = to_mate(w_part.at[slot, w_rows], w_other.at[slot, w_rows], swap_send.at[0, slot], swap_recv.at[0, slot])
                swap.start()
                g_swap.wait()
                gram = g_part[slot] + g_other[slot]
                t_rows = buf[z, pl.ds(y, 2), :, tiles].reshape(BLOCK, TILE)
                t_1 = merged(t_rows[:HALF], group, gram[:HALF, :HALF])
                t_2 = merged(t_rows[HALF:], group, gram[HALF:, HALF:])
                cross = gram[:HALF, HALF:]
                run('mid')
                swap.wait()
                w_t = w_part[slot, w_rows] + w_other[slot, w_rows]

            y_2 = dot_nt(w_t[:, HALF:], t_2)
            y_1 = dot_nt(w_t[:, :HALF] - dot_nt(y_2, cross), t_1)
            y_t = jnp.concatenate([y_1, y_2], axis=1)

            def update(tile, count):
                x_buf[:, rows_of(tile, count)] -= dot_nn(y_t, block_of(tile, count))

            over_rows(update)
            return carry

        lax.fori_loop(0, 8, block_step, 0)

    apply_group(2)
    apply_group(1)
    apply_group(0)
    out_ref[...] = x_buf[...]

    give.wait_send()
    swap_line.wait_send()
    give_half.wait_send()
    for kind in range(4):
        for copy in line_copies(kind, False):
            copy.wait_send()
    for key in message_keys():
        for copy in messages(*key, False):
            copy.wait_send()


def solution(mesh):
    def local_apply(v_loc, t_loc, z_loc):
        groups, width = t_loc.shape[0], t_loc.shape[1]
        local_rows = v_loc.shape[0]
        cols = 2 * z_loc.shape[1]
        t_tile = jnp.pad(t_loc.transpose(1, 0, 2).reshape(width, groups * width), ((0, 0), (0, TILE - groups * width)))
        any_spec = pl.BlockSpec(memory_space=pl.ANY)
        dma = pltpu.SemaphoreType.DMA

        def vmem(*shape):
            return pltpu.VMEM(shape, jnp.float32)

        x_t = pl.pallas_call(
            kernel,
            out_shape=jax.ShapeDtypeStruct((cols, local_rows), jnp.float32),
            in_specs=[any_spec, any_spec, any_spec],
            out_specs=pl.BlockSpec(memory_space=pltpu.VMEM),
            scratch_shapes=[
                *(vmem(SIDE, SIDE, SIDE, TILES[group] + EXTRA[group], WIDTH, TILE) for group in (2, 1, 0)),
                vmem(SIDE, SIDE, SIDE, len(OWNERS), WIDTH, TILE),
                vmem(cols, local_rows),
                vmem(2, cols + HALF, BLOCK), vmem(2, cols + HALF, BLOCK),
                vmem(2, BLOCK, BLOCK), vmem(2, BLOCK, BLOCK),
                *(vmem(SIDE, WIDTH, QUARTERS[group]) for group in OWNERS), vmem(SIDE, WIDTH, TILE),
                vmem(2, HALF, HALF), vmem(2, HALF, HALF), vmem(SIDE, 2, HALF // 2, HALF),
                vmem(2, HALF, HALF), vmem(2, HALF, HALF),
                dma((3,)), dma((3,)), dma((len(TABLE),)), dma((len(TABLE),)), dma((2, 2)), dma((2, 2)),
                dma((5, 3)), dma((5, 3)), dma((3,)),
            ],
            compiler_params=pltpu.CompilerParams(collective_id=0, has_side_effects=True, vmem_limit_bytes=67043328),
        )(v_loc.T, t_tile, z_loc.T)
        return x_t.T

    return jax.shard_map(local_apply, mesh=mesh,
                         in_specs=(P('row', 'col'), P('col', None, None), P(None, ('col', 'row'))),
                         out_specs=P('row', 'col'), check_vma=False)
```

```python
import jax
import jax.numpy as jnp
from jax import lax
from jax.experimental import pallas as pl
from jax.experimental.pallas import tpu as pltpu
from jax.sharding import PartitionSpec as P

HIGHEST = lax.Precision.HIGHEST
MESH = pl.DeviceIdType.MESH
BLOCK = 256
HALF = BLOCK // 2
TILE = 128
SIDE = 4
WIDTH = 32
TILES = {2: 8, 1: 16, 0: 24}
OWNERS = (1, 0)
QUARTERS = {group: TILES[group] // SIDE * TILE for group in OWNERS}
ORDERS = ((2, 1, 0), (1, 0, 2), (0, 2, 1))
RANGES = {
    2: ((8, 9), (0, 5), (5, 8)),
    1: ((14, 17), (0, 7), (7, 14)),
    0: ((20, 25), (0, 12), (12, 20)),
}
PRELUDE = (
    'b200.b201.b202.r1.f200.f202.f201.e202.b212',
    'e201.b211.e200.b210.m11.f212.m12.f210.f211',
    'e210.e212.b2223.b220.r0.b2222.m13.m14.f2223',
    'b100.b101.b102.e211.b2213.f2213.e2213.b2212.f2222',
    'f220.b2211.f100.e2223.m01.f102.b2221.f2212.f101',
    'm02.f2211.e2222.e220',
)
EVENTS = {
    (2, 'before'): {1: 'm03', 3: 'f111', 4: 'f001', 5: 'e112.e000.b1223.b010.e110.b120', 6: 'f1213.f1223.f1212.f120.b1222.b1210.f1211.f010.e2210', 7: 'b1221'},
    (2, 'mid'): {0: 'e102.b112.b2220.e100.b110.f2221.e2212', 1: 'e101.b111.m04.e2211.b000.b001.b002.f2220', 2: 'f112.f110', 3: 'e2221.f000', 4: 'f002.b2210.e2220', 5: 'e111.e001.b1213.b1212.b1211.b011.f2210.e002', 6: 'e1213.e1223.e1212', 7: 'f1222.f011.f1210.b012'},
    (1, 'before'): {0: 'e010.e1211.b1220.f1221.e1210.e120', 1: 'f012.b020', 2: 'e011', 3: 'e012', 4: 'f0213.e1221', 5: 'e1220', 6: 'f0223.f0212', 7: 'b0222'},
    (1, 'mid'): {1: 'e1222', 2: 'f1220.b0213', 4: 'f020.b0223.b0212', 5: 'e0213', 7: 'b0211'},
    (0, 'before'): {0: 'e0223.e0212.f0222.e020', 1: 'b0221', 4: 'e0221', 6: 'e0220'},
    (0, 'mid'): {0: 'f0211', 1: 'e0222.b0210', 2: 'f0221.e0211', 3: 'f0210.b0220', 4: 'f0220', 5: 'e0210'},
}


def dot_nn(a, b):
    return lax.dot_general(a, b, (((1,), (0,)), ((), ())), precision=HIGHEST, preferred_element_type=jnp.float32)


def dot_nt(a, b):
    return lax.dot_general(a, b, (((1,), (1,)), ((), ())), precision=HIGHEST, preferred_element_type=jnp.float32)


def regions(group, part, phase, plane, coords, pos, half):
    order = ORDERS[part]
    low, high = RANGES[group][part]
    index = list(coords)
    index[order[phase]] = pos
    for axis in order[:phase]:
        index[axis] = pl.ds(0, SIDE)
    if phase == 0:
        middle = (low + high + 1) // 2
        low, high = ((low, middle), (middle, high))[half]
    else:
        index[order[1 if plane is not None and order[0] == 0 else 0]] = pl.ds(2 * half, 2)
    if plane is not None:
        index[0] = plane
        low = max(low, 2 * plane)
    return (*index, pl.ds(low, high - low)) if low < high else None


def planes_of(part, phase):
    return (3, 2, 1, 0) if part and phase == 2 else (None,)


def message_keys():
    for group in TILES:
        for phase in range(3):
            for part in range(3):
                for plane in planes_of(part, phase):
                    for piece in range(3):
                        yield group, phase, part, plane, piece


def half_of(piece, way):
    return 1 - way if piece == 1 else way


def semaphore_table():
    table = {}
    for group, phase, part, plane, piece in message_keys():
        for way in range(2):
            if regions(group, part, phase, plane, (0, 0, 0), 0, half_of(piece, way)) is not None:
                table[group, phase, part, plane, piece, way] = len(table)
    return table


TABLE = semaphore_table()


def kernel(v_hbm, t_hbm, z_hbm, out_ref, buf2, buf1, buf0, x_buf, w_part, w_other, g_part, g_other, quarters_1,
           quarters_0, t_line,
           line_part, line_other, line_half, line_gram, line_t,
           load_sem, x_sem, send_sem, recv_sem, swap_send, swap_recv, line_send, line_recv, line_load):
    bufs = {2: buf2, 1: buf1, 0: buf0}
    quarters = {1: quarters_1, 0: quarters_0}
    cols, local_rows = x_buf.shape
    share = cols // 2
    me = lax.axis_index('row')
    mate = 1 - me
    chip = lax.axis_index('col')
    coords = (chip // (SIDE * SIDE), lax.rem(chip // SIDE, SIDE), lax.rem(chip, SIDE))
    strides = (SIDE * SIDE, SIDE, 1)
    my_x = coords[2]

    def shifted(axis, by):
        return lax.rem(coords[axis] + by + SIDE, SIDE)

    def neighbour(axis, by):
        return {'col': chip + (shifted(axis, by) - coords[axis]) * strides[axis]}

    def to_mate(src, dst, send, recv):
        return pltpu.make_async_remote_copy(src_ref=src, dst_ref=dst, send_sem=send, recv_sem=recv,
                                            device_id={'row': mate}, device_id_type=MESH)

    for group in TILES:
        for z in range(1, SIDE):
            shape = (SIDE, SIDE, 2 * z, WIDTH, TILE)
            bufs[group][z, :, :, 0:2 * z, :, :] = jnp.zeros(shape, jnp.float32)

    barrier = pltpu.get_barrier_semaphore()
    pl.semaphore_signal(barrier, inc=1, device_id={'row': mate}, device_id_type=MESH)
    for axis, by in ((0, 1), (0, -1), (1, 1), (1, -1), (2, 1), (2, 2), (2, 3)):
        pl.semaphore_signal(barrier, inc=1, device_id=neighbour(axis, by), device_id_type=MESH)
    pl.semaphore_wait(barrier, 8)

    own = {group: bufs[group].at[coords[0], coords[1], coords[2]] for group in TILES}

    def load(group):
        first = local_rows - TILES[group] * TILE
        for tile in range(TILES[group]):
            src = v_hbm.at[pl.ds(group * WIDTH, WIDTH), pl.ds(first + tile * TILE, TILE)]
            pltpu.make_async_copy(src, own[group].at[tile], load_sem.at[group]).start()
        if group == 2:
            pltpu.make_async_copy(t_hbm, own[2].at[TILES[2]], load_sem.at[2]).start()

    def loaded(group):
        tiles = pl.ds(0, TILES[group] + (1 if group == 2 else 0))
        pltpu.make_async_copy(own[group].at[tiles], own[group].at[tiles], load_sem.at[group]).wait()

    mine = pl.ds(pl.multiple_of(me * local_rows, TILE), local_rows)
    theirs = pl.ds(pl.multiple_of(mate * local_rows, TILE), local_rows)
    my_cols = x_buf.at[pl.ds(pl.multiple_of(me * share, 8), share), :]
    their_cols = x_buf.at[pl.ds(pl.multiple_of(mate * share, 8), share), :]
    keep = pltpu.make_async_copy(z_hbm.at[:, mine], my_cols, x_sem.at[0])
    give = to_mate(z_hbm.at[:, theirs], my_cols, x_sem.at[1], x_sem.at[2])
    take = to_mate(z_hbm.at[:, theirs], their_cols, x_sem.at[1], x_sem.at[2])

    def messages(group, phase, part, plane, piece, incoming):
        copies = []
        axis = ORDERS[part][phase]
        for way in range(2):
            sign = 1 - 2 * way
            pos = shifted(axis, (-sign if piece == 2 else 0) + (-sign if incoming else 0))
            index = regions(group, part, phase, plane, coords, pos, half_of(piece, way))
            if index is None:
                continue
            number = TABLE[group, phase, part, plane, piece, way]
            ref = bufs[group].at[index]
            copies.append(pltpu.make_async_remote_copy(
                src_ref=ref, dst_ref=ref, send_sem=send_sem.at[number], recv_sem=recv_sem.at[number],
                device_id=neighbour(axis, sign), device_id_type=MESH))
        return copies

    def begin(group, phase, part, plane=None):
        for piece in range(2):
            for copy in messages(group, phase, part, plane, piece, False):
                copy.start()

    def forward(group, phase, part, plane=None):
        for copy in messages(group, phase, part, plane, 0, True):
            copy.wait_recv()
        for copy in messages(group, phase, part, plane, 2, False):
            copy.start()

    def finish(group, phase, part, plane=None):
        for piece in range(1, 3):
            for copy in messages(group, phase, part, plane, piece, True):
                copy.wait_recv()

    def quarter(group, x):
        first = local_rows - TILES[group] * TILE
        lanes = pl.ds(pl.multiple_of(first + x * QUARTERS[group], TILE), QUARTERS[group])
        return v_hbm.at[pl.ds(group * WIDTH, WIDTH), lanes]

    def line_copies(kind, i, incoming):
        copies = []
        for by in range(1, SIDE):
            slot = shifted(2, -by) if incoming else my_x
            if kind == 0:
                src, dst = quarter(OWNERS[i], shifted(2, by)), quarters[OWNERS[i]].at[slot]
            elif kind == 1:
                src, dst = line_half.at[i, my_x], line_half.at[i, slot]
            else:
                src, dst = t_hbm, t_line.at[slot]
            copies.append(pltpu.make_async_remote_copy(
                src_ref=src, dst_ref=dst, send_sem=line_send.at[i, kind, by - 1], recv_sem=line_recv.at[i, kind, by - 1],
                device_id=neighbour(2, by), device_id_type=MESH))
        return copies

    own_quarters = [pltpu.make_async_copy(quarter(group, my_x), quarters[group].at[my_x], line_load.at[i])
                    for i, group in enumerate(OWNERS)]
    own_t = pltpu.make_async_copy(t_hbm, t_line.at[my_x], line_load.at[2])
    my_half = pl.ds(pl.multiple_of(me * (HALF // 2), 8), HALF // 2)
    their_half = pl.ds(pl.multiple_of(mate * (HALF // 2), 8), HALF // 2)

    def swap_line(i):
        return to_mate(line_part.at[i], line_other.at[i], line_send.at[i, 3, 0], line_recv.at[i, 3, 0])

    def swap_half(i, half):
        return to_mate(line_gram.at[i, my_half], line_gram.at[i, half], line_send.at[i, 3, 1], line_recv.at[i, 3, 1])

    def block_diagonal(t_rows, group):
        size = t_rows.shape[0]
        column = t_rows[:, group * WIDTH:(group + 1) * WIDTH]
        wide = jnp.concatenate([column] * (size // WIDTH), axis=1)
        row_id = lax.broadcasted_iota(jnp.int32, (size, size), 0)
        col_id = lax.broadcasted_iota(jnp.int32, (size, size), 1)
        return jnp.where(row_id // WIDTH == col_id // WIDTH, wide, 0.0), row_id, col_id

    def merged(t_rows, group, gram):
        t_mat, row_id, col_id = block_diagonal(t_rows, group)
        size = WIDTH
        while size < gram.shape[0]:
            pick = (row_id // size + 1 == col_id // size) & (row_id // (2 * size) == col_id // (2 * size))
            t_mat = t_mat - dot_nn(dot_nn(t_mat, jnp.where(pick, gram, 0.0)), t_mat)
            size *= 2
        return t_mat

    def trade(group):
        i = OWNERS.index(group)
        own_quarters[i].start()
        for copy in line_copies(0, i, False):
            copy.start()
        if i == 0:
            own_t.start()
            for copy in line_copies(2, i, False):
                copy.start()

    def merge(group, stage):
        i = OWNERS.index(group)
        if stage == 1:
            for copy in line_copies(0, i, True):
                copy.wait_recv()
            own_quarters[i].wait()
            rows = quarters[group][...].reshape(HALF, QUARTERS[group])
            line_part[i] = dot_nt(rows, rows)
            swap_line(i).start()
        elif stage == 2:
            swap_line(i).wait_recv()
            line_half[i, my_x] = line_part[i, my_half] + line_other[i, my_half]
            for copy in line_copies(1, i, False):
                copy.start()
        elif stage == 3:
            for copy in line_copies(1, i, True):
                copy.wait_recv()
            line_gram[i, my_half] = (line_half[i, 0] + line_half[i, 1]) + (line_half[i, 2] + line_half[i, 3])
            swap_half(i, my_half).start()
        else:
            swap_half(i, their_half).wait_recv()
            if i == 0:
                own_t.wait()
                for copy in line_copies(2, i, True):
                    copy.wait_recv()
            line_t[i] = merged(t_line[...].reshape(HALF, TILE), group, line_gram[i])
            mine = pl.ds(pl.multiple_of(my_x * WIDTH, 8), WIDTH)
            bufs[group][coords[0], coords[1], coords[2], TILES[group]] = line_t[i, mine]

    actions = {'b': begin, 'f': forward, 'e': finish, 'r': trade, 'm': merge}

    def act(events):
        for event in events.split('.'):
            actions[event[0]](*(int(digit) for digit in event[1:]))

    for group in TILES:
        load(group)
    keep.start()
    give.start()
    for group in TILES:
        loaded(group)
    for events in PRELUDE:
        act(events)
    keep.wait()
    take.wait_recv()

    def apply_group(group):
        buf = bufs[group]
        tiles = TILES[group]
        first_row = local_rows - tiles * TILE

        def block_step(step, carry):
            blk = 7 - step
            z, y = blk // 2, 2 * lax.rem(blk, 2)
            slot = lax.rem(step, 2)

            def run(where):
                for when, events in EVENTS.get((group, where), {}).items():
                    @pl.when(step == when)
                    def _():
                        act(events)

            def block_of(tile, count):
                pieces = [buf[z, pl.ds(y, 2), :, tile + i].reshape(BLOCK, TILE) for i in range(count)]
                return jnp.concatenate(pieces, axis=1)

            def rows_of(tile, count):
                return pl.ds(pl.multiple_of(first_row + tile * TILE, TILE), count * TILE)

            def over_rows(body):
                @pl.when(blk >= 4)
                def _():
                    body(4, 4)

                lax.fori_loop(blk // 4, tiles // 8, lambda c, carry: (body(8 * c, 8), carry)[1], 0)

            run('before')
            if group in OWNERS:
                w_part[slot] = jnp.zeros(w_part.shape[1:], jnp.float32)

                def products(tile, count):
                    v_c = block_of(tile, count)
                    x_c = x_buf[:, rows_of(tile, count)]
                    w_part[slot] += dot_nt(jnp.concatenate([x_c, v_c[:HALF]], axis=0), v_c)

                over_rows(products)
                swap = to_mate(w_part.at[slot], w_other.at[slot], swap_send.at[0, slot], swap_recv.at[0, slot])
                swap.start()
                run('mid')
                swap.wait()
                total = w_part[slot] + w_other[slot]
                w_t, cross = total[:cols], total[cols:, HALF:]
                t_1 = buf[z, y, :, tiles].reshape(HALF, HALF)
                t_2 = buf[z, y + 1, :, tiles].reshape(HALF, HALF)
            else:
                g_part[slot] = jnp.zeros(g_part.shape[1:], jnp.float32)

                def gram_products(tile, count):
                    v_c = block_of(tile, count)
                    g_part[slot] += dot_nt(v_c, v_c)

                over_rows(gram_products)
                g_swap = to_mate(g_part.at[slot], g_other.at[slot], swap_send.at[1, slot], swap_recv.at[1, slot])
                g_swap.start()
                w_rows = pl.ds(0, cols)
                w_part[slot, w_rows] = jnp.zeros((cols, BLOCK), jnp.float32)

                def w_products(tile, count):
                    w_part[slot, w_rows] += dot_nt(x_buf[:, rows_of(tile, count)], block_of(tile, count))

                over_rows(w_products)
                swap = to_mate(w_part.at[slot, w_rows], w_other.at[slot, w_rows], swap_send.at[0, slot], swap_recv.at[0, slot])
                swap.start()
                g_swap.wait()
                gram = g_part[slot] + g_other[slot]
                t_rows = buf[z, pl.ds(y, 2), :, tiles].reshape(BLOCK, TILE)
                t_1 = merged(t_rows[:HALF], group, gram[:HALF, :HALF])
                t_2 = merged(t_rows[HALF:], group, gram[HALF:, HALF:])
                cross = gram[:HALF, HALF:]
                run('mid')
                swap.wait()
                w_t = w_part[slot, w_rows] + w_other[slot, w_rows]

            y_2 = dot_nt(w_t[:, HALF:], t_2)
            y_1 = dot_nt(w_t[:, :HALF] - dot_nt(y_2, cross), t_1)
            y_t = jnp.concatenate([y_1, y_2], axis=1)

            def update(tile, count):
                x_buf[:, rows_of(tile, count)] -= dot_nn(y_t, block_of(tile, count))

            over_rows(update)
            return carry

        lax.fori_loop(0, 8, block_step, 0)

    apply_group(2)
    apply_group(1)
    apply_group(0)
    out_ref[...] = x_buf[...]

    give.wait_send()
    for i in range(len(OWNERS)):
        swap_line(i).wait_send()
        swap_half(i, my_half).wait_send()
        for kind in range(3 if i == 0 else 2):
            for copy in line_copies(kind, i, False):
                copy.wait_send()
    for key in message_keys():
        for copy in messages(*key, False):
            copy.wait_send()


def solution(mesh):
    def local_apply(v_loc, t_loc, z_loc):
        groups, width = t_loc.shape[0], t_loc.shape[1]
        local_rows = v_loc.shape[0]
        cols = 2 * z_loc.shape[1]
        t_tile = jnp.pad(t_loc.transpose(1, 0, 2).reshape(width, groups * width), ((0, 0), (0, TILE - groups * width)))
        any_spec = pl.BlockSpec(memory_space=pl.ANY)
        dma = pltpu.SemaphoreType.DMA

        def vmem(*shape):
            return pltpu.VMEM(shape, jnp.float32)

        x_t = pl.pallas_call(
            kernel,
            out_shape=jax.ShapeDtypeStruct((cols, local_rows), jnp.float32),
            in_specs=[any_spec, any_spec, any_spec],
            out_specs=pl.BlockSpec(memory_space=pltpu.VMEM),
            scratch_shapes=[
                *(vmem(SIDE, SIDE, SIDE, TILES[group] + 1, WIDTH, TILE) for group in (2, 1, 0)),
                vmem(cols, local_rows),
                vmem(2, cols + HALF, BLOCK), vmem(2, cols + HALF, BLOCK),
                vmem(2, BLOCK, BLOCK), vmem(2, BLOCK, BLOCK),
                *(vmem(SIDE, WIDTH, QUARTERS[group]) for group in OWNERS), vmem(SIDE, WIDTH, TILE),
                vmem(2, HALF, HALF), vmem(2, HALF, HALF), vmem(2, SIDE, HALF // 2, HALF),
                vmem(2, HALF, HALF), vmem(2, HALF, HALF),
                dma((3,)), dma((3,)), dma((len(TABLE),)), dma((len(TABLE),)), dma((2, 2)), dma((2, 2)),
                dma((2, 4, 3)), dma((2, 4, 3)), dma((3,)),
            ],
            compiler_params=pltpu.CompilerParams(collective_id=0, has_side_effects=True, vmem_limit_bytes=67043328),
        )(v_loc.T, t_tile, z_loc.T)
        return x_t.T

    return jax.shard_map(local_apply, mesh=mesh,
                         in_specs=(P('row', 'col'), P('col', None, None), P(None, ('col', 'row'))),
                         out_specs=P('row', 'col'), check_vma=False)
```

```python
import jax
import jax.numpy as jnp
from jax import lax
from jax.experimental import pallas as pl
from jax.experimental.pallas import tpu as pltpu
from jax.sharding import PartitionSpec as P

HIGHEST = lax.Precision.HIGHEST
MESH = pl.DeviceIdType.MESH
BLOCK = 256
HALF = BLOCK // 2
TILE = 128
SIDE = 4
WIDTH = 32
TILES = {2: 8, 1: 16, 0: 24}
OWNERS = (1, 0)
QUARTERS = {group: TILES[group] // SIDE * TILE for group in OWNERS}
ORDERS = ((2, 1, 0), (1, 0, 2), (0, 2, 1))
RANGES = {
    2: ((7, 9), (0, 5), (5, 7)),
    1: ((14, 17), (0, 9), (9, 14)),
    0: ((21, 25), (0, 11), (11, 21)),
}
PRELUDE = (
    'b200.b201.b202.r1.f200.f202.f201.e202.b212',
    'r0.e201.b211.e200.b210.m11.f212.m12.f211',
    'f210.e210.b220.e211.b2213.f2213.e2213.b2212.b2211',
    'm01.e212.b2223.b2222.m02.m13.f2212.b2221.m14',
    'f2223.b100.b101.b102.f2211.f220.f2222.b2210.m03',
    'e2212.f2221.f100.m04.b002.e2223.e2211.f102.b2220',
    'f101.b001.f2210.e2222.e2221.f2220.e100.b110.b000',
    'e220',
)
EVENTS = {
    (2, 'before'): {1: 'f000.e102.b112', 2: 'e2220', 4: 'e112', 6: 'f1223', 7: 'f120.b1213.b011'},
    (2, 'mid'): {0: 'f002.e101.b111.e2210', 1: 'f001.e002.e000.b010', 2: 'f110.f112.b012.f111', 3: 'e001.f010', 4: 'b1223.e110.b120', 5: 'f012.e010.e111.b1222', 7: 'f1222.b1212'},
    (1, 'before'): {0: 'e012.f1213.b1221.e1223.e1222.f1212.b1220.f1221.b1211.e120.e1213', 1: 'e1212', 6: 'b0222.f020.e1210'},
    (1, 'mid'): {1: 'f1220.f011.f1211', 2: 'b1210.b0223.e1221', 3: 'e1211.e1220.b020', 4: 'e011.f1210.f0223', 5: 'b0213', 6: 'e0223.b0212.f0213', 7: 'f0222'},
    (0, 'before'): {0: 'f0212.b0211.b0221.e0213.e020', 3: 'e0211', 4: 'f0210', 6: 'e0210.e0220'},
    (0, 'mid'): {0: 'e0222.e0212', 1: 'f0211.f0221', 2: 'b0210.b0220', 3: 'e0221', 4: 'f0220'},
}


def dot_nn(a, b):
    return lax.dot_general(a, b, (((1,), (0,)), ((), ())), precision=HIGHEST, preferred_element_type=jnp.float32)


def dot_nt(a, b):
    return lax.dot_general(a, b, (((1,), (1,)), ((), ())), precision=HIGHEST, preferred_element_type=jnp.float32)


def regions(group, part, phase, plane, coords, pos, half):
    order = ORDERS[part]
    low, high = RANGES[group][part]
    index = list(coords)
    index[order[phase]] = pos
    for axis in order[:phase]:
        index[axis] = pl.ds(0, SIDE)
    if phase == 0:
        middle = (low + high + 1) // 2
        low, high = ((low, middle), (middle, high))[half]
    else:
        index[order[1 if plane is not None and order[0] == 0 else 0]] = pl.ds(2 * half, 2)
    if plane is not None:
        index[0] = plane
        low = max(low, 2 * plane + (half if part == 1 else 0))
    return (*index, pl.ds(low, high - low)) if low < high else None


def planes_of(part, phase):
    return (3, 2, 1, 0) if part and phase == 2 else (None,)


def message_keys():
    for group in TILES:
        for phase in range(3):
            for part in range(3):
                for plane in planes_of(part, phase):
                    for piece in range(3):
                        yield group, phase, part, plane, piece


def half_of(piece, way):
    return 1 - way if piece == 1 else way


def semaphore_table():
    table = {}
    for group, phase, part, plane, piece in message_keys():
        for way in range(2):
            if regions(group, part, phase, plane, (0, 0, 0), 0, half_of(piece, way)) is not None:
                table[group, phase, part, plane, piece, way] = len(table)
    return table


TABLE = semaphore_table()


def kernel(v_hbm, t_hbm, z_hbm, out_ref, buf2, buf1, buf0, x_buf, w_part, w_other, g_part, g_other, quarters_1,
           quarters_0, t_line,
           line_part, line_other, line_half, line_gram, line_t,
           load_sem, x_sem, send_sem, recv_sem, swap_send, swap_recv, line_send, line_recv, line_load):
    bufs = {2: buf2, 1: buf1, 0: buf0}
    quarters = {1: quarters_1, 0: quarters_0}
    cols, local_rows = x_buf.shape
    share = cols // 2
    me = lax.axis_index('row')
    mate = 1 - me
    chip = lax.axis_index('col')
    coords = (chip // (SIDE * SIDE), lax.rem(chip // SIDE, SIDE), lax.rem(chip, SIDE))
    strides = (SIDE * SIDE, SIDE, 1)
    my_x = coords[2]

    def shifted(axis, by):
        return lax.rem(coords[axis] + by + SIDE, SIDE)

    def neighbour(axis, by):
        return {'col': chip + (shifted(axis, by) - coords[axis]) * strides[axis]}

    def to_mate(src, dst, send, recv):
        return pltpu.make_async_remote_copy(src_ref=src, dst_ref=dst, send_sem=send, recv_sem=recv,
                                            device_id={'row': mate}, device_id_type=MESH)

    for group in TILES:
        for blk in range(1, 2 * SIDE):
            z, y = blk // 2, 2 * (blk % 2)
            bufs[group][z, y:y + 2, :, 0:blk, :, :] = jnp.zeros((2, SIDE, blk, WIDTH, TILE), jnp.float32)

    own = {group: bufs[group].at[coords[0], coords[1], coords[2]] for group in TILES}

    def load(group):
        first = local_rows - TILES[group] * TILE
        for tile in range(TILES[group]):
            src = v_hbm.at[pl.ds(group * WIDTH, WIDTH), pl.ds(first + tile * TILE, TILE)]
            pltpu.make_async_copy(src, own[group].at[tile], load_sem.at[group]).start()
        if group == 2:
            pltpu.make_async_copy(t_hbm, own[2].at[TILES[2]], load_sem.at[2]).start()

    def loaded(group):
        tiles = pl.ds(0, TILES[group] + (1 if group == 2 else 0))
        pltpu.make_async_copy(own[group].at[tiles], own[group].at[tiles], load_sem.at[group]).wait()

    for group in TILES:
        load(group)

    barrier = pltpu.get_barrier_semaphore()
    pl.semaphore_signal(barrier, inc=1, device_id={'row': mate}, device_id_type=MESH)
    for axis, by in ((0, 1), (0, -1), (1, 1), (1, -1), (2, 1), (2, 2), (2, 3)):
        pl.semaphore_signal(barrier, inc=1, device_id=neighbour(axis, by), device_id_type=MESH)
    pl.semaphore_wait(barrier, 8)

    mine = pl.ds(pl.multiple_of(me * local_rows, TILE), local_rows)
    theirs = pl.ds(pl.multiple_of(mate * local_rows, TILE), local_rows)
    my_cols = x_buf.at[pl.ds(pl.multiple_of(me * share, 8), share), :]
    their_cols = x_buf.at[pl.ds(pl.multiple_of(mate * share, 8), share), :]
    keep = pltpu.make_async_copy(z_hbm.at[:, mine], my_cols, x_sem.at[0])
    give = to_mate(z_hbm.at[:, theirs], my_cols, x_sem.at[1], x_sem.at[2])
    take = to_mate(z_hbm.at[:, theirs], their_cols, x_sem.at[1], x_sem.at[2])

    def messages(group, phase, part, plane, piece, incoming):
        copies = []
        axis = ORDERS[part][phase]
        for way in range(2):
            sign = 1 - 2 * way
            pos = shifted(axis, (-sign if piece == 2 else 0) + (-sign if incoming else 0))
            index = regions(group, part, phase, plane, coords, pos, half_of(piece, way))
            if index is None:
                continue
            number = TABLE[group, phase, part, plane, piece, way]
            ref = bufs[group].at[index]
            copies.append(pltpu.make_async_remote_copy(
                src_ref=ref, dst_ref=ref, send_sem=send_sem.at[number], recv_sem=recv_sem.at[number],
                device_id=neighbour(axis, sign), device_id_type=MESH))
        return copies

    def begin(group, phase, part, plane=None):
        with jax.named_scope(f"begin#g={group}#p={phase}#a={part}#z={plane}"):
            for piece in range(2):
                for copy in messages(group, phase, part, plane, piece, False):
                    copy.start()

    def forward(group, phase, part, plane=None):
        with jax.named_scope(f"forward#g={group}#p={phase}#a={part}#z={plane}"):
            for copy in messages(group, phase, part, plane, 0, True):
                copy.wait_recv()
            for copy in messages(group, phase, part, plane, 2, False):
                copy.start()

    def finish(group, phase, part, plane=None):
        with jax.named_scope(f"finish#g={group}#p={phase}#a={part}#z={plane}"):
            for piece in range(1, 3):
                for copy in messages(group, phase, part, plane, piece, True):
                    copy.wait_recv()

    def quarter(group, x):
        first = local_rows - TILES[group] * TILE
        lanes = pl.ds(pl.multiple_of(first + x * QUARTERS[group], TILE), QUARTERS[group])
        return v_hbm.at[pl.ds(group * WIDTH, WIDTH), lanes]

    def line_copies(kind, i, incoming):
        copies = []
        for by in range(1, SIDE):
            slot = shifted(2, -by) if incoming else my_x
            if kind == 0:
                src, dst = quarter(OWNERS[i], shifted(2, by)), quarters[OWNERS[i]].at[slot]
            elif kind == 1:
                src, dst = line_half.at[i, my_x], line_half.at[i, slot]
            else:
                src, dst = t_hbm, t_line.at[slot]
            copies.append(pltpu.make_async_remote_copy(
                src_ref=src, dst_ref=dst, send_sem=line_send.at[i, kind, by - 1], recv_sem=line_recv.at[i, kind, by - 1],
                device_id=neighbour(2, by), device_id_type=MESH))
        return copies

    own_quarters = [pltpu.make_async_copy(quarter(group, my_x), quarters[group].at[my_x], line_load.at[i])
                    for i, group in enumerate(OWNERS)]
    own_t = pltpu.make_async_copy(t_hbm, t_line.at[my_x], line_load.at[2])
    my_half = pl.ds(pl.multiple_of(me * (HALF // 2), 8), HALF // 2)
    their_half = pl.ds(pl.multiple_of(mate * (HALF // 2), 8), HALF // 2)

    def swap_line(i):
        return to_mate(line_part.at[i], line_other.at[i], line_send.at[i, 3, 0], line_recv.at[i, 3, 0])

    def swap_half(i, half):
        return to_mate(line_gram.at[i, my_half], line_gram.at[i, half], line_send.at[i, 3, 1], line_recv.at[i, 3, 1])

    def block_diagonal(t_rows, group):
        size = t_rows.shape[0]
        column = t_rows[:, group * WIDTH:(group + 1) * WIDTH]
        wide = jnp.concatenate([column] * (size // WIDTH), axis=1)
        row_id = lax.broadcasted_iota(jnp.int32, (size, size), 0)
        col_id = lax.broadcasted_iota(jnp.int32, (size, size), 1)
        return jnp.where(row_id // WIDTH == col_id // WIDTH, wide, 0.0), row_id, col_id

    def merged(t_rows, group, gram):
        t_mat, row_id, col_id = block_diagonal(t_rows, group)
        size = WIDTH
        while size < gram.shape[0]:
            pick = (row_id // size + 1 == col_id // size) & (row_id // (2 * size) == col_id // (2 * size))
            t_mat = t_mat - dot_nn(dot_nn(t_mat, jnp.where(pick, gram, 0.0)), t_mat)
            size *= 2
        return t_mat

    def trade(group):
        i = OWNERS.index(group)
        own_quarters[i].start()
        for copy in line_copies(0, i, False):
            copy.start()
        if i == 0:
            own_t.start()
            for copy in line_copies(2, i, False):
                copy.start()

    def merge(group, stage):
        with jax.named_scope(f"merge#g={group}#s={stage}"):
            i = OWNERS.index(group)
            if stage == 1:
                for copy in line_copies(0, i, True):
                    copy.wait_recv()
                own_quarters[i].wait()
                rows = quarters[group][...].reshape(HALF, QUARTERS[group])
                line_part[i] = dot_nt(rows, rows)
                swap_line(i).start()
            elif stage == 2:
                swap_line(i).wait_recv()
                line_half[i, my_x] = line_part[i, my_half] + line_other[i, my_half]
                for copy in line_copies(1, i, False):
                    copy.start()
            elif stage == 3:
                for copy in line_copies(1, i, True):
                    copy.wait_recv()
                line_gram[i, my_half] = (line_half[i, 0] + line_half[i, 1]) + (line_half[i, 2] + line_half[i, 3])
                swap_half(i, my_half).start()
            else:
                swap_half(i, their_half).wait_recv()
                if i == 0:
                    own_t.wait()
                    for copy in line_copies(2, i, True):
                        copy.wait_recv()
                line_t[i] = merged(t_line[...].reshape(HALF, TILE), group, line_gram[i])
                mine = pl.ds(pl.multiple_of(my_x * WIDTH, 8), WIDTH)
                bufs[group][coords[0], coords[1], coords[2], TILES[group]] = line_t[i, mine]

    actions = {'b': begin, 'f': forward, 'e': finish, 'r': trade, 'm': merge}

    def act(events):
        for event in events.split('.'):
            actions[event[0]](*(int(digit) for digit in event[1:]))

    keep.start()
    give.start()
    for group in TILES:
        loaded(group)
    for events in PRELUDE:
        act(events)
    keep.wait()
    take.wait_recv()

    def apply_group(group):
        buf = bufs[group]
        tiles = TILES[group]
        first_row = local_rows - tiles * TILE

        def block_step(step, carry):
            blk = 7 - step
            z, y = blk // 2, 2 * lax.rem(blk, 2)
            slot = lax.rem(step, 2)

            def run(where):
                for when, events in EVENTS.get((group, where), {}).items():
                    @pl.when(step == when)
                    def _():
                        act(events)

            def block_of(tile, count):
                pieces = [buf[z, pl.ds(y, 2), :, tile + i].reshape(BLOCK, TILE) for i in range(count)]
                return jnp.concatenate(pieces, axis=1)

            def rows_of(tile, count):
                return pl.ds(pl.multiple_of(first_row + tile * TILE, TILE), count * TILE)

            def over_rows(body):
                @pl.when(blk >= 4)
                def _():
                    body(4, 4)

                lax.fori_loop(blk // 4, tiles // 8, lambda c, carry: (body(8 * c, 8), carry)[1], 0)

            run('before')
            if group in OWNERS:
                w_part[slot] = jnp.zeros(w_part.shape[1:], jnp.float32)

                def products(tile, count):
                    v_c = block_of(tile, count)
                    x_c = x_buf[:, rows_of(tile, count)]
                    w_part[slot] += dot_nt(jnp.concatenate([x_c, v_c[:HALF]], axis=0), v_c)

                with jax.named_scope('products'):
                    over_rows(products)
                swap = to_mate(w_part.at[slot], w_other.at[slot], swap_send.at[0, slot], swap_recv.at[0, slot])
                swap.start()
                run('mid')
                with jax.named_scope('swapwait'):
                    swap.wait()
                total = w_part[slot] + w_other[slot]
                w_t, cross = total[:cols], total[cols:, HALF:]
                t_1 = buf[z, y, :, tiles].reshape(HALF, HALF)
                t_2 = buf[z, y + 1, :, tiles].reshape(HALF, HALF)
            else:
                g_part[slot] = jnp.zeros(g_part.shape[1:], jnp.float32)

                def gram_products(tile, count):
                    v_c = block_of(tile, count)
                    g_part[slot] += dot_nt(v_c, v_c)

                with jax.named_scope('gram'):
                    over_rows(gram_products)
                g_swap = to_mate(g_part.at[slot], g_other.at[slot], swap_send.at[1, slot], swap_recv.at[1, slot])
                g_swap.start()
                w_rows = pl.ds(0, cols)
                w_part[slot, w_rows] = jnp.zeros((cols, BLOCK), jnp.float32)

                def w_products(tile, count):
                    w_part[slot, w_rows] += dot_nt(x_buf[:, rows_of(tile, count)], block_of(tile, count))

                over_rows(w_products)
                swap = to_mate(w_part.at[slot, w_rows], w_other.at[slot, w_rows], swap_send.at[0, slot], swap_recv.at[0, slot])
                swap.start()
                g_swap.wait()
                gram = g_part[slot] + g_other[slot]
                t_rows = buf[z, pl.ds(y, 2), :, tiles].reshape(BLOCK, TILE)
                t_1 = merged(t_rows[:HALF], group, gram[:HALF, :HALF])
                t_2 = merged(t_rows[HALF:], group, gram[HALF:, HALF:])
                cross = gram[:HALF, HALF:]
                run('mid')
                with jax.named_scope('swapwait'):
                    swap.wait()
                w_t = w_part[slot, w_rows] + w_other[slot, w_rows]

            y_2 = dot_nt(w_t[:, HALF:], t_2)
            y_1 = dot_nt(w_t[:, :HALF] - dot_nt(y_2, cross), t_1)
            y_t = jnp.concatenate([y_1, y_2], axis=1)

            def update(tile, count):
                x_buf[:, rows_of(tile, count)] -= dot_nn(y_t, block_of(tile, count))

            with jax.named_scope('update'):
                over_rows(update)
            return carry

        lax.fori_loop(0, 8, block_step, 0)

    apply_group(2)
    apply_group(1)
    apply_group(0)
    out_ref[...] = x_buf[...]

    give.wait_send()
    for i in range(len(OWNERS)):
        swap_line(i).wait_send()
        swap_half(i, my_half).wait_send()
        for kind in range(3 if i == 0 else 2):
            for copy in line_copies(kind, i, False):
                copy.wait_send()
    for key in message_keys():
        for copy in messages(*key, False):
            copy.wait_send()


def solution(mesh):
    def local_apply(v_loc, t_loc, z_loc):
        groups, width = t_loc.shape[0], t_loc.shape[1]
        local_rows = v_loc.shape[0]
        cols = 2 * z_loc.shape[1]
        t_tile = jnp.pad(t_loc.transpose(1, 0, 2).reshape(width, groups * width), ((0, 0), (0, TILE - groups * width)))
        any_spec = pl.BlockSpec(memory_space=pl.ANY)
        dma = pltpu.SemaphoreType.DMA

        def vmem(*shape):
            return pltpu.VMEM(shape, jnp.float32)

        x_t = pl.pallas_call(
            kernel,
            out_shape=jax.ShapeDtypeStruct((cols, local_rows), jnp.float32),
            in_specs=[any_spec, any_spec, any_spec],
            out_specs=pl.BlockSpec(memory_space=pltpu.VMEM),
            scratch_shapes=[
                *(vmem(SIDE, SIDE, SIDE, TILES[group] + 1, WIDTH, TILE) for group in (2, 1, 0)),
                vmem(cols, local_rows),
                vmem(2, cols + HALF, BLOCK), vmem(2, cols + HALF, BLOCK),
                vmem(2, BLOCK, BLOCK), vmem(2, BLOCK, BLOCK),
                *(vmem(SIDE, WIDTH, QUARTERS[group]) for group in OWNERS), vmem(SIDE, WIDTH, TILE),
                vmem(2, HALF, HALF), vmem(2, HALF, HALF), vmem(2, SIDE, HALF // 2, HALF),
                vmem(2, HALF, HALF), vmem(2, HALF, HALF),
                dma((3,)), dma((3,)), dma((len(TABLE),)), dma((len(TABLE),)), dma((2, 2)), dma((2, 2)),
                dma((2, 4, 3)), dma((2, 4, 3)), dma((3,)),
            ],
            compiler_params=pltpu.CompilerParams(collective_id=0, has_side_effects=True, vmem_limit_bytes=67043328),
        )(v_loc.T, t_tile, z_loc.T)
        return x_t.T

    return jax.shard_map(local_apply, mesh=mesh,
                         in_specs=(P('row', 'col'), P('col', None, None), P(None, ('col', 'row'))),
                         out_specs=P('row', 'col'), check_vma=False)
```

```python
import jax
import jax.numpy as jnp
from jax import lax
from jax.experimental import pallas as pl
from jax.experimental.pallas import tpu as pltpu
from jax.sharding import PartitionSpec as P

HIGHEST = lax.Precision.HIGHEST
MESH = pl.DeviceIdType.MESH
BLOCK = 256
HALF = BLOCK // 2
TILE = 128
SIDE = 4
WIDTH = 32
TILES = {2: 8, 1: 16, 0: 24}
OWNERS = (1, 0)
QUARTERS = {group: TILES[group] // SIDE * TILE for group in OWNERS}
ORDERS = ((2, 1, 0), (1, 0, 2), (0, 2, 1))
RANGES = {
    2: ((7, 9), (0, 5), (5, 7)),
    1: ((14, 17), (0, 9), (9, 14)),
    0: ((21, 25), (0, 11), (11, 21)),
}
PRELUDE = (
    'b201.b200.b202.r1.f200.f202.f201.e202.b212',
    'r0.e201.b211.e200.b210.m11.f212.m12.f210',
    'f211.e210.b220.e211.b2213.f2213.e2213.b2212.b2211',
    'm01.e212.b2223.b2222.m02.m13.f2212.b2221.m14',
    'f2223.b101.b100.b102.f2211.f220.f2222.b2210.m03',
    'e2212.f2221.f100.m04.b000.b002.e2223.e2211.f102',
    'b2220.f101.f2210.e2222.e2221.f2220.e100.b110.e220',
)
EVENTS = {
    (2, 'before'): {1: 'e102.b112.e2210.e2220', 4: 'e112.b1223', 6: 'b1213', 7: 'f1222'},
    (2, 'mid'): {0: 'f000.f002.e101.b111', 1: 'e000.b010.e002.f110', 2: 'f112.b012.f010.f111.b001', 3: 'e110.b120', 4: 'f001.e010.b1222', 5: 'e111.f1223.f012', 6: 'e001.b1212.b1221.f120', 7: 'b1211.e012'},
    (1, 'before'): {0: ('f1213.e1223.b1220.b011.f1212.f1221.e120', 'b1210.e1222.f1211.f1220.f011.e1213'), 1: 'e1212.e1221', 2: 'f1210.b020', 3: 'e011.f0223', 4: 'e1211', 5: 'e1210.f020', 6: 'b0212'},
    (1, 'mid'): {0: 'b0223', 1: 'e1220', 4: 'b0213.b0222', 5: 'f0213.e0223', 6: 'f0222.e0213', 7: 'f0212'},
    (0, 'before'): {0: 'b0211.b0221.e020', 3: 'e0211', 4: 'f0210', 6: 'e0210.e0220'},
    (0, 'mid'): {0: 'e0212.e0222', 1: 'f0211.f0221', 2: 'b0210.b0220', 3: 'e0221', 4: 'f0220'},
}


def dot_nn(a, b):
    return lax.dot_general(a, b, (((1,), (0,)), ((), ())), precision=HIGHEST, preferred_element_type=jnp.float32)


def dot_nt(a, b):
    return lax.dot_general(a, b, (((1,), (1,)), ((), ())), precision=HIGHEST, preferred_element_type=jnp.float32)


def regions(group, part, phase, plane, coords, pos, half):
    order = ORDERS[part]
    low, high = RANGES[group][part]
    index = list(coords)
    index[order[phase]] = pos
    for axis in order[:phase]:
        index[axis] = pl.ds(0, SIDE)
    if phase == 0:
        middle = (low + high + 1) // 2
        low, high = ((low, middle), (middle, high))[half]
    else:
        index[order[1 if plane is not None and order[0] == 0 else 0]] = pl.ds(2 * half, 2)
    if plane is not None:
        index[0] = plane
        low = max(low, 2 * plane + (half if part == 1 else 0))
    return (*index, pl.ds(low, high - low)) if low < high else None


def planes_of(part, phase):
    return (3, 2, 1, 0) if part and phase == 2 else (None,)


def message_keys():
    for group in TILES:
        for phase in range(3):
            for part in range(3):
                for plane in planes_of(part, phase):
                    for piece in range(3):
                        yield group, phase, part, plane, piece


def half_of(piece, way):
    return 1 - way if piece == 1 else way


def semaphore_table():
    table = {}
    for group, phase, part, plane, piece in message_keys():
        for way in range(2):
            if regions(group, part, phase, plane, (0, 0, 0), 0, half_of(piece, way)) is not None:
                table[group, phase, part, plane, piece, way] = len(table)
    return table


TABLE = semaphore_table()


def kernel(v_hbm, t_hbm, z_hbm, out_ref, buf2, buf1, buf0, x_buf, w_part, w_other, g_part, g_other, quarters_1,
           quarters_0, t_line,
           line_part, line_other, line_half, line_gram, line_t,
           load_sem, x_sem, send_sem, recv_sem, swap_send, swap_recv, line_send, line_recv, line_load):
    bufs = {2: buf2, 1: buf1, 0: buf0}
    quarters = {1: quarters_1, 0: quarters_0}
    cols, local_rows = x_buf.shape
    share = cols // 2
    me = lax.axis_index('row')
    mate = 1 - me
    chip = lax.axis_index('col')
    coords = (chip // (SIDE * SIDE), lax.rem(chip // SIDE, SIDE), lax.rem(chip, SIDE))
    strides = (SIDE * SIDE, SIDE, 1)
    my_x = coords[2]

    def shifted(axis, by):
        return lax.rem(coords[axis] + by + SIDE, SIDE)

    def neighbour(axis, by):
        return {'col': chip + (shifted(axis, by) - coords[axis]) * strides[axis]}

    def to_mate(src, dst, send, recv):
        return pltpu.make_async_remote_copy(src_ref=src, dst_ref=dst, send_sem=send, recv_sem=recv,
                                            device_id={'row': mate}, device_id_type=MESH)

    for group in TILES:
        for blk in range(1, 2 * SIDE):
            z, y = blk // 2, 2 * (blk % 2)
            bufs[group][z, y:y + 2, :, 0:blk, :, :] = jnp.zeros((2, SIDE, blk, WIDTH, TILE), jnp.float32)

    own = {group: bufs[group].at[coords[0], coords[1], coords[2]] for group in TILES}

    def load(group):
        first = local_rows - TILES[group] * TILE
        for tile in range(TILES[group]):
            src = v_hbm.at[pl.ds(group * WIDTH, WIDTH), pl.ds(first + tile * TILE, TILE)]
            pltpu.make_async_copy(src, own[group].at[tile], load_sem.at[group]).start()
        if group == 2:
            pltpu.make_async_copy(t_hbm, own[2].at[TILES[2]], load_sem.at[2]).start()

    def loaded(group):
        tiles = pl.ds(0, TILES[group] + (1 if group == 2 else 0))
        pltpu.make_async_copy(own[group].at[tiles], own[group].at[tiles], load_sem.at[group]).wait()

    for group in TILES:
        load(group)

    barrier = pltpu.get_barrier_semaphore()
    pl.semaphore_signal(barrier, inc=1, device_id={'row': mate}, device_id_type=MESH)
    for axis, by in ((0, 1), (0, -1), (1, 1), (1, -1), (2, 1), (2, 2), (2, 3)):
        pl.semaphore_signal(barrier, inc=1, device_id=neighbour(axis, by), device_id_type=MESH)
    pl.semaphore_wait(barrier, 8)

    mine = pl.ds(pl.multiple_of(me * local_rows, TILE), local_rows)
    theirs = pl.ds(pl.multiple_of(mate * local_rows, TILE), local_rows)
    my_cols = x_buf.at[pl.ds(pl.multiple_of(me * share, 8), share), :]
    their_cols = x_buf.at[pl.ds(pl.multiple_of(mate * share, 8), share), :]
    keep = pltpu.make_async_copy(z_hbm.at[:, mine], my_cols, x_sem.at[0])
    give = to_mate(z_hbm.at[:, theirs], my_cols, x_sem.at[1], x_sem.at[2])
    take = to_mate(z_hbm.at[:, theirs], their_cols, x_sem.at[1], x_sem.at[2])

    def messages(group, phase, part, plane, piece, incoming):
        copies = []
        axis = ORDERS[part][phase]
        for way in range(2):
            sign = 1 - 2 * way
            pos = shifted(axis, (-sign if piece == 2 else 0) + (-sign if incoming else 0))
            index = regions(group, part, phase, plane, coords, pos, half_of(piece, way))
            if index is None:
                continue
            number = TABLE[group, phase, part, plane, piece, way]
            ref = bufs[group].at[index]
            copies.append(pltpu.make_async_remote_copy(
                src_ref=ref, dst_ref=ref, send_sem=send_sem.at[number], recv_sem=recv_sem.at[number],
                device_id=neighbour(axis, sign), device_id_type=MESH))
        return copies

    def begin(group, phase, part, plane=None):
        for piece in range(2):
            for copy in messages(group, phase, part, plane, piece, False):
                copy.start()

    def forward(group, phase, part, plane=None):
        for copy in messages(group, phase, part, plane, 0, True):
            copy.wait_recv()
        for copy in messages(group, phase, part, plane, 2, False):
            copy.start()

    def finish(group, phase, part, plane=None):
        for piece in range(1, 3):
            for copy in messages(group, phase, part, plane, piece, True):
                copy.wait_recv()

    def quarter(group, x):
        first = local_rows - TILES[group] * TILE
        lanes = pl.ds(pl.multiple_of(first + x * QUARTERS[group], TILE), QUARTERS[group])
        return v_hbm.at[pl.ds(group * WIDTH, WIDTH), lanes]

    def line_copies(kind, i, incoming):
        copies = []
        for by in range(1, SIDE):
            slot = shifted(2, -by) if incoming else my_x
            if kind == 0:
                src, dst = quarter(OWNERS[i], shifted(2, by)), quarters[OWNERS[i]].at[slot]
            elif kind == 1:
                src, dst = line_half.at[i, my_x], line_half.at[i, slot]
            else:
                src, dst = t_hbm, t_line.at[slot]
            copies.append(pltpu.make_async_remote_copy(
                src_ref=src, dst_ref=dst, send_sem=line_send.at[i, kind, by - 1], recv_sem=line_recv.at[i, kind, by - 1],
                device_id=neighbour(2, by), device_id_type=MESH))
        return copies

    own_quarters = [pltpu.make_async_copy(quarter(group, my_x), quarters[group].at[my_x], line_load.at[i])
                    for i, group in enumerate(OWNERS)]
    own_t = pltpu.make_async_copy(t_hbm, t_line.at[my_x], line_load.at[2])
    my_half = pl.ds(pl.multiple_of(me * (HALF // 2), 8), HALF // 2)
    their_half = pl.ds(pl.multiple_of(mate * (HALF // 2), 8), HALF // 2)

    def swap_line(i):
        return to_mate(line_part.at[i], line_other.at[i], line_send.at[i, 3, 0], line_recv.at[i, 3, 0])

    def swap_half(i, half):
        return to_mate(line_gram.at[i, my_half], line_gram.at[i, half], line_send.at[i, 3, 1], line_recv.at[i, 3, 1])

    def block_diagonal(t_rows, group):
        size = t_rows.shape[0]
        column = t_rows[:, group * WIDTH:(group + 1) * WIDTH]
        wide = jnp.concatenate([column] * (size // WIDTH), axis=1)
        row_id = lax.broadcasted_iota(jnp.int32, (size, size), 0)
        col_id = lax.broadcasted_iota(jnp.int32, (size, size), 1)
        return jnp.where(row_id // WIDTH == col_id // WIDTH, wide, 0.0), row_id, col_id

    def merged(t_rows, group, gram):
        t_mat, row_id, col_id = block_diagonal(t_rows, group)
        size = WIDTH
        while size < gram.shape[0]:
            pick = (row_id // size + 1 == col_id // size) & (row_id // (2 * size) == col_id // (2 * size))
            t_mat = t_mat - dot_nn(dot_nn(t_mat, jnp.where(pick, gram, 0.0)), t_mat)
            size *= 2
        return t_mat

    def trade(group):
        i = OWNERS.index(group)
        own_quarters[i].start()
        for copy in line_copies(0, i, False):
            copy.start()
        if i == 0:
            own_t.start()
            for copy in line_copies(2, i, False):
                copy.start()

    def merge(group, stage):
        i = OWNERS.index(group)
        if stage == 1:
            for copy in line_copies(0, i, True):
                copy.wait_recv()
            own_quarters[i].wait()
            rows = quarters[group][...].reshape(HALF, QUARTERS[group])
            line_part[i] = dot_nt(rows, rows)
            swap_line(i).start()
        elif stage == 2:
            swap_line(i).wait_recv()
            line_half[i, my_x] = line_part[i, my_half] + line_other[i, my_half]
            for copy in line_copies(1, i, False):
                copy.start()
        elif stage == 3:
            for copy in line_copies(1, i, True):
                copy.wait_recv()
            line_gram[i, my_half] = (line_half[i, 0] + line_half[i, 1]) + (line_half[i, 2] + line_half[i, 3])
            swap_half(i, my_half).start()
        else:
            swap_half(i, their_half).wait_recv()
            if i == 0:
                own_t.wait()
                for copy in line_copies(2, i, True):
                    copy.wait_recv()
            line_t[i] = merged(t_line[...].reshape(HALF, TILE), group, line_gram[i])
            mine = pl.ds(pl.multiple_of(my_x * WIDTH, 8), WIDTH)
            bufs[group][coords[0], coords[1], coords[2], TILES[group]] = line_t[i, mine]

    actions = {'b': begin, 'f': forward, 'e': finish, 'r': trade, 'm': merge}

    def act(events):
        for event in events.split('.'):
            actions[event[0]](*(int(digit) for digit in event[1:]))

    keep.start()
    give.start()
    for group in TILES:
        loaded(group)
    for events in PRELUDE:
        act(events)
    keep.wait()
    take.wait_recv()

    def apply_group(group):
        buf = bufs[group]
        tiles = TILES[group]
        first_row = local_rows - tiles * TILE

        def block_step(step, carry):
            blk = 7 - step
            z, y = blk // 2, 2 * lax.rem(blk, 2)
            slot = lax.rem(step, 2)

            def run(where):
                for when, events in EVENTS.get((group, where), {}).items():
                    @pl.when(step == when)
                    def _():
                        for some in events if isinstance(events, tuple) else (events,):
                            act(some)

            def block_of(tile, count):
                pieces = [buf[z, pl.ds(y, 2), :, tile + i].reshape(BLOCK, TILE) for i in range(count)]
                return jnp.concatenate(pieces, axis=1)

            def rows_of(tile, count):
                return pl.ds(pl.multiple_of(first_row + tile * TILE, TILE), count * TILE)

            def over_rows(body):
                @pl.when(blk >= 4)
                def _():
                    body(4, 4)

                lax.fori_loop(blk // 4, tiles // 8, lambda c, carry: (body(8 * c, 8), carry)[1], 0)

            run('before')
            if group in OWNERS:
                w_part[slot] = jnp.zeros(w_part.shape[1:], jnp.float32)

                def products(tile, count):
                    v_c = block_of(tile, count)
                    x_c = x_buf[:, rows_of(tile, count)]
                    w_part[slot] += dot_nt(jnp.concatenate([x_c, v_c[:HALF]], axis=0), v_c)

                over_rows(products)
                swap = to_mate(w_part.at[slot], w_other.at[slot], swap_send.at[0, slot], swap_recv.at[0, slot])
                swap.start()
                run('mid')
                swap.wait()
                total = w_part[slot] + w_other[slot]
                w_t, cross = total[:cols], total[cols:, HALF:]
                t_1 = buf[z, y, :, tiles].reshape(HALF, HALF)
                t_2 = buf[z, y + 1, :, tiles].reshape(HALF, HALF)
            else:
                g_part[slot] = jnp.zeros(g_part.shape[1:], jnp.float32)

                def gram_products(tile, count):
                    v_c = block_of(tile, count)
                    g_part[slot] += dot_nt(v_c, v_c)

                over_rows(gram_products)
                g_swap = to_mate(g_part.at[slot], g_other.at[slot], swap_send.at[1, slot], swap_recv.at[1, slot])
                g_swap.start()
                w_rows = pl.ds(0, cols)
                w_part[slot, w_rows] = jnp.zeros((cols, BLOCK), jnp.float32)

                def w_products(tile, count):
                    w_part[slot, w_rows] += dot_nt(x_buf[:, rows_of(tile, count)], block_of(tile, count))

                over_rows(w_products)
                swap = to_mate(w_part.at[slot, w_rows], w_other.at[slot, w_rows], swap_send.at[0, slot], swap_recv.at[0, slot])
                swap.start()
                g_swap.wait()
                gram = g_part[slot] + g_other[slot]
                t_rows = buf[z, pl.ds(y, 2), :, tiles].reshape(BLOCK, TILE)
                t_1 = merged(t_rows[:HALF], group, gram[:HALF, :HALF])
                t_2 = merged(t_rows[HALF:], group, gram[HALF:, HALF:])
                cross = gram[:HALF, HALF:]
                run('mid')
                swap.wait()
                w_t = w_part[slot, w_rows] + w_other[slot, w_rows]

            y_2 = dot_nt(w_t[:, HALF:], t_2)
            y_1 = dot_nt(w_t[:, :HALF] - dot_nt(y_2, cross), t_1)
            y_t = jnp.concatenate([y_1, y_2], axis=1)

            def update(tile, count):
                x_buf[:, rows_of(tile, count)] -= dot_nn(y_t, block_of(tile, count))

            over_rows(update)
            return carry

        lax.fori_loop(0, 8, block_step, 0)

    apply_group(2)
    apply_group(1)
    apply_group(0)
    out_ref[...] = x_buf[...]

    give.wait_send()
    for i in range(len(OWNERS)):
        swap_line(i).wait_send()
        swap_half(i, my_half).wait_send()
        for kind in range(3 if i == 0 else 2):
            for copy in line_copies(kind, i, False):
                copy.wait_send()
    for key in message_keys():
        for copy in messages(*key, False):
            copy.wait_send()


def solution(mesh):
    def local_apply(v_loc, t_loc, z_loc):
        groups, width = t_loc.shape[0], t_loc.shape[1]
        local_rows = v_loc.shape[0]
        cols = 2 * z_loc.shape[1]
        t_tile = jnp.pad(t_loc.transpose(1, 0, 2).reshape(width, groups * width), ((0, 0), (0, TILE - groups * width)))
        any_spec = pl.BlockSpec(memory_space=pl.ANY)
        dma = pltpu.SemaphoreType.DMA

        def vmem(*shape):
            return pltpu.VMEM(shape, jnp.float32)

        x_t = pl.pallas_call(
            kernel,
            out_shape=jax.ShapeDtypeStruct((cols, local_rows), jnp.float32),
            in_specs=[any_spec, any_spec, any_spec],
            out_specs=pl.BlockSpec(memory_space=pltpu.VMEM),
            scratch_shapes=[
                *(vmem(SIDE, SIDE, SIDE, TILES[group] + 1, WIDTH, TILE) for group in (2, 1, 0)),
                vmem(cols, local_rows),
                vmem(2, cols + HALF, BLOCK), vmem(2, cols + HALF, BLOCK),
                vmem(2, BLOCK, BLOCK), vmem(2, BLOCK, BLOCK),
                *(vmem(SIDE, WIDTH, QUARTERS[group]) for group in OWNERS), vmem(SIDE, WIDTH, TILE),
                vmem(2, HALF, HALF), vmem(2, HALF, HALF), vmem(2, SIDE, HALF // 2, HALF),
                vmem(2, HALF, HALF), vmem(2, HALF, HALF),
                dma((3,)), dma((3,)), dma((len(TABLE),)), dma((len(TABLE),)), dma((2, 2)), dma((2, 2)),
                dma((2, 4, 3)), dma((2, 4, 3)), dma((3,)),
            ],
            compiler_params=pltpu.CompilerParams(collective_id=0, has_side_effects=True, vmem_limit_bytes=67043328),
        )(v_loc.T, t_tile, z_loc.T)
        return x_t.T

    return jax.shard_map(local_apply, mesh=mesh,
                         in_specs=(P('row', 'col'), P('col', None, None), P(None, ('col', 'row'))),
                         out_specs=P('row', 'col'), check_vma=False)
```
